32 devices in a mesh: cells: 32 (over z, y, x, core).
Axes of the slice: x: 2, y: 2, z: 4, core: 2. Of those that a mesh axis runs over, the one named last changes fastest.
Arguments:
- field: float32 [9, 55, 32768], P(None, None, 'cells'), may hold values from -6 to 6
- cell_area: float32 [32768], P('cells'), may hold values from 0.5 to 2
- dv_edge: float32 [103424], P('cells'), may hold values from 0.6 to 1.6
- dc_edge: float32 [103424], P('cells'), may hold values from 0.6 to 1.6
- cells_on_edge: int32 [2, 103424], P(None, 'cells'), may hold values from 0 to 1407, as said below
- edges_on_cell: int32 [6, 32768], P(None, 'cells'), may hold values from 0 to 3231, as said below
- send_cells: int32 [6, 2048], P(None, 'cells'), may hold values from 0 to 1023
- level_coef: float32 [55], replicated, may hold values from 0.005 to 0.02
Outputs:
- tendency: float32 [9, 55, 32768], P(None, None, 'cells')
The draws below stay inside these ranges and needn't reach their ends.
Inputs may be any that keep to these rules, and one draw needn't show every extreme that they name: `cells_on_edge`: the blocks tile one periodic hexagonal mesh, each a parallelogram of 64 by 16 cells; block b borders b + 1 and b - 1 along the first direction, b + 16 and b - 16 along the second, and b + 15 and b - 15 at one cell each, all modulo 32. Every edge with a cell in a block is listed once in that block, with the same dv_edge and dc_edge wherever it is listed, plus one extra entry that no cell names. Cells and edges are numbered in random order in each block. `edges_on_cell`: each cell names six distinct edges of its block.
All inputs are finite; a program needn't handle non-finite values.
Results may differ from the reference program's by a relative error of at most 0.00005.
Values sent between devices are 32-bit elements; how exact they have to be, the bound alone decides.
A program may use at most 128 MiB of HBM per device.

```python
import math
import jax
import jax.numpy as jnp
import numpy as np
from jax import lax

CELLS_X = 64
CELLS_Y = 16
FIELDS = 9
LEVELS = 55
BLOCK_ROW = 16
BLOCKS = 32
CELLS_DEV = 1024
SLOT = 64
EDGES_DEV = 3232
TOTAL_CELLS = 32768


def canonical_tables():
    width = CELLS_X
    height = CELLS_Y
    cell_count = width * height
    places = np.arange(cell_count)
    column = places % width
    row_index = places // width
    step_x = np.array([1, 0, 1])
    step_y = np.array([0, 1, -1])
    owned_dir = np.tile(np.arange(3), cell_count)
    owned_sx = np.repeat(column, 3)
    owned_sy = np.repeat(row_index, 3)
    owned_tx = owned_sx + step_x[owned_dir]
    owned_ty = owned_sy + step_y[owned_dir]
    along_y = np.arange(height)
    along_x = np.arange(width)
    short_x = np.arange(width - 1)
    src_x = np.concatenate([owned_sx, -np.ones(height, np.int64), -np.ones(height, np.int64), along_x, short_x, np.zeros(1, np.int64)])
    src_y = np.concatenate([owned_sy, along_y, along_y + 1, -np.ones(width, np.int64), height * np.ones(width - 1, np.int64), np.zeros(1, np.int64)])
    dst_x = np.concatenate([owned_tx, np.zeros(height, np.int64), np.zeros(height, np.int64), along_x, short_x + 1, np.zeros(1, np.int64)])
    dst_y = np.concatenate([owned_ty, along_y, along_y, np.zeros(width, np.int64), (height - 1) * np.ones(width - 1, np.int64), np.zeros(1, np.int64)])
    edge_dir = np.concatenate([owned_dir, np.zeros(height, np.int64), 2 * np.ones(height, np.int64), np.ones(width, np.int64), 2 * np.ones(width - 1, np.int64), np.zeros(1, np.int64)])
    base = 3 * cell_count
    beside_all = np.stack([places * 3, places * 3 + 1, places * 3 + 2, np.where(column > 0, (places - 1) * 3, base + row_index), np.where(row_index > 0, (places - width) * 3 + 1, base + 2 * height + column), np.where((column > 0) & (row_index < height - 1), (places + width - 1) * 3 + 2, np.where(column == 0, base + height + row_index, base + 2 * height + width + column - 1))])
    return (src_x, src_y, dst_x, dst_y, edge_dir, beside_all)


def frame_slots(coord_x, coord_y):
    width = CELLS_X
    height = CELLS_Y
    cell_count = width * height
    slot_len = CELLS_X
    inside_y = (coord_y >= 0) & (coord_y < height)
    inside_x = (coord_x >= 0) & (coord_x < width)
    is_own = inside_x & inside_y
    own_place = np.clip(coord_y, 0, height - 1) * width + np.clip(coord_x, 0, width - 1)
    halo_index = np.where((coord_x == -1) & inside_y, cell_count + coord_y, np.where((coord_x == width) & inside_y, cell_count + slot_len + coord_y, np.where((coord_y == -1) & inside_x, cell_count + 2 * slot_len + coord_x, np.where((coord_y == height) & inside_x, cell_count + 3 * slot_len + coord_x, np.where((coord_x == width) & (coord_y == -1), cell_count + 4 * slot_len + 0 * coord_x, np.where((coord_x == -1) & (coord_y == height), cell_count + 5 * slot_len + 0 * coord_x, 0))))))
    return (is_own, own_place, halo_index)


def mesh_numbering(key):
    cell_keys = jax.random.split(jax.random.fold_in(key, 11), BLOCKS)
    edge_keys = jax.random.split(jax.random.fold_in(key, 12), BLOCKS)
    place_of_cell = jax.vmap(lambda sub: jax.random.permutation(sub, CELLS_DEV))(cell_keys).astype(jnp.int32)
    cell_of_place = jnp.argsort(place_of_cell, axis=1).astype(jnp.int32)
    canon_of_edge = jax.vmap(lambda sub: jax.random.permutation(sub, EDGES_DEV))(edge_keys).astype(jnp.int32)
    edge_of_canon = jnp.argsort(canon_of_edge, axis=1).astype(jnp.int32)
    return (place_of_cell, cell_of_place, canon_of_edge, edge_of_canon)


def draw_cells_on_edge(key, part):
    src_x, src_y, dst_x, dst_y, edge_dir, beside_all = canonical_tables()
    place_of_cell, cell_of_place, canon_of_edge, edge_of_canon = mesh_numbering(key)
    results = []
    for coord_x, coord_y in ((src_x, src_y), (dst_x, dst_y)):
        is_own, own_place, halo_index = frame_slots(coord_x, coord_y)
        own_local = jnp.take(cell_of_place, jnp.asarray(own_place, jnp.int32), axis=1)
        canon_value = jnp.where(jnp.asarray(is_own)[None, :], own_local, jnp.asarray(halo_index, jnp.int32)[None, :])
        results.append(jnp.take_along_axis(canon_value, canon_of_edge, axis=1))
    return jnp.stack(results).reshape(2, BLOCKS * EDGES_DEV).astype(jnp.int32)


def draw_edges_on_cell(key, part):
    src_x, src_y, dst_x, dst_y, edge_dir, beside_all = canonical_tables()
    place_of_cell, cell_of_place, canon_of_edge, edge_of_canon = mesh_numbering(key)
    canon_edges = jnp.take(jnp.asarray(beside_all, jnp.int32), place_of_cell, axis=1)
    local_edges = jnp.take_along_axis(jnp.broadcast_to(edge_of_canon, (6, BLOCKS, EDGES_DEV)), canon_edges, axis=2)
    return local_edges.reshape(6, BLOCKS * CELLS_DEV).astype(jnp.int32)


def draw_send_cells(key, part):
    width = CELLS_X
    height = CELLS_Y
    place_of_cell, cell_of_place, canon_of_edge, edge_of_canon = mesh_numbering(key)
    entry = np.arange(CELLS_X)
    short = np.minimum(entry, height - 1)
    positions = np.stack([short * width + width - 1, short * width, (height - 1) * width + entry, entry, (height - 1) * width + 0 * entry, width - 1 + 0 * entry])
    limits = np.array([height, height, width, width, 1, 1])
    valid = entry[None, :] < limits[:, None]
    chosen = jnp.take(cell_of_place, jnp.asarray(positions, jnp.int32), axis=1)
    chosen = jnp.where(jnp.asarray(valid)[None, :, :], chosen, 0)
    return jnp.transpose(chosen, (1, 0, 2)).reshape(6, BLOCKS * SLOT).astype(jnp.int32)


def edge_global_ids(key):
    src_x, src_y, dst_x, dst_y, edge_dir, beside_all = canonical_tables()
    place_of_cell, cell_of_place, canon_of_edge, edge_of_canon = mesh_numbering(key)
    block_x = src_x // CELLS_X
    block_y = src_y // CELLS_Y
    src_place = src_y % CELLS_Y * CELLS_X + src_x % CELLS_X
    block_step = jnp.asarray(block_x + BLOCK_ROW * block_y, jnp.int32)
    block_ids = lax.broadcasted_iota(jnp.int32, (BLOCKS, EDGES_DEV), 0)
    owner = jnp.mod(block_ids + block_step[None, :], BLOCKS)
    global_ids = (owner * CELLS_DEV + jnp.asarray(src_place, jnp.int32)[None, :]) * 3 + jnp.asarray(edge_dir, jnp.int32)[None, :]
    return jnp.take_along_axis(global_ids, canon_of_edge, axis=1).reshape(BLOCKS * EDGES_DEV)


def draw_dv_edge(key, part):
    sub = jax.random.fold_in(key, 21)
    count = BLOCKS * CELLS_DEV * 3
    table = jnp.exp(jax.random.uniform(sub, (count,), jnp.float32, math.log(0.7), math.log(1.4)))
    return jnp.take(table, edge_global_ids(key)).astype(jnp.float32)


def draw_dc_edge(key, part):
    sub = jax.random.fold_in(key, 22)
    count = BLOCKS * CELLS_DEV * 3
    table = jnp.exp(jax.random.uniform(sub, (count,), jnp.float32, math.log(0.7), math.log(1.4)))
    return jnp.take(table, edge_global_ids(key)).astype(jnp.float32)


def level_of(stream_key, shape, cuts, least, high):
    level = 1.0
    for axis_at, blocks in cuts:
        steps = jax.random.uniform(jax.random.fold_in(jax.random.fold_in(stream_key, 6), axis_at), (blocks,), jnp.float32, least / len(cuts), high / len(cuts))
        level = level * jnp.repeat(jnp.exp(steps), shape[axis_at] // blocks).reshape((-1,) + (1,) * (len(shape) - 1 - axis_at))
    return level


def bell_draw(key, shape, scale, most, cuts=(), held_as=jnp.bfloat16):
    values = scale * jax.random.normal(key, shape, jnp.float32)
    if cuts:
        values = values * level_of(key, shape, cuts, -0.22, 0.18)
    return jnp.clip(values, -most, most).astype(held_as)


def setup_inputs(seed: int = 0) -> dict:
    arg_keys = jax.random.split(jax.random.key(seed), 9)
    field = bell_draw(arg_keys[0], (FIELDS, LEVELS, TOTAL_CELLS), 1.0, 6.0, ((2, 32),), jnp.float32)
    cell_area = jnp.clip(jnp.exp(math.log(2.0) - 1.3862944 * jax.random.uniform(arg_keys[1], (TOTAL_CELLS,), jnp.float32) ** level_of(arg_keys[1], (TOTAL_CELLS,), ((0, 32),), -0.2, 0.2)), 0.5, 2.0)
    dv_edge = draw_dv_edge(jax.random.fold_in(arg_keys[8], 71), 0)
    dc_edge = draw_dc_edge(jax.random.fold_in(arg_keys[8], 71), 0)
    cells_on_edge = draw_cells_on_edge(jax.random.fold_in(arg_keys[8], 71), 0)
    edges_on_cell = draw_edges_on_cell(jax.random.fold_in(arg_keys[8], 71), 0)
    send_cells = draw_send_cells(jax.random.fold_in(arg_keys[8], 71), 0)
    level_coef = jnp.clip(jnp.exp(jax.random.uniform(arg_keys[7], (LEVELS,), jnp.float32, math.log(0.005), math.log(0.02))), 0.005, 0.02)
    return {"field": field, "cell_area": cell_area, "dv_edge": dv_edge, "dc_edge": dc_edge, "cells_on_edge": cells_on_edge, "edges_on_cell": edges_on_cell, "send_cells": send_cells, "level_coef": level_coef}


def reference(field, cell_area, dv_edge, dc_edge, cells_on_edge, edges_on_cell, send_cells, level_coef):
    blocks = BLOCKS
    weight = (dv_edge / dc_edge).reshape(blocks, EDGES_DEV)
    area_block = cell_area.reshape(blocks, CELLS_DEV)
    endpoints = cells_on_edge.reshape(2, blocks, EDGES_DEV)
    beside_all = edges_on_cell.reshape(6, blocks, CELLS_DEV)
    send_lists = send_cells.reshape(6, blocks, SLOT)
    offsets = (1, -1, BLOCK_ROW, -BLOCK_ROW, BLOCK_ROW - 1, 1 - BLOCK_ROW)
    first_end = jnp.take_along_axis(jnp.broadcast_to(endpoints[0], (6, blocks, EDGES_DEV)), beside_all, axis=2)
    own_index = lax.broadcasted_iota(jnp.int32, (6, blocks, CELLS_DEV), 2)
    orient = jnp.where(first_end == own_index, 1.0, -1.0).astype(jnp.float32)

    def laplacian(values):
        pieces = [values]
        for direction in range(6):
            source = jnp.roll(values, offsets[direction], axis=0)
            chosen = jnp.roll(send_lists[direction], offsets[direction], axis=0)
            pieces.append(jnp.take_along_axis(source, chosen, axis=1))
        extended = jnp.concatenate(pieces, axis=1)
        upper_end = jnp.take_along_axis(extended, endpoints[1], axis=1)
        lower_end = jnp.take_along_axis(extended, endpoints[0], axis=1)
        fluxes = weight * (upper_end - lower_end)
        gathered = jnp.take_along_axis(jnp.broadcast_to(fluxes, (6, blocks, EDGES_DEV)), beside_all, axis=2)
        return jnp.sum(orient * gathered, axis=0) / area_block

    def one_level(packed):
        values, factor = packed
        return -factor * laplacian(laplacian(values))

    level_rows = field.reshape(FIELDS * LEVELS, blocks, CELLS_DEV)
    factors = jnp.tile(level_coef, FIELDS)
    result = lax.map(one_level, (level_rows, factors))
    return result.reshape(FIELDS, LEVELS, blocks * CELLS_DEV)
```

```python
import functools

import jax
import jax.numpy as jnp
from jax import lax
from jax.experimental import pallas as pl
from jax.experimental.pallas import tpu as pltpu
from jax.sharding import PartitionSpec as P

CELLS_Y = 16
BLOCK_ROW = 16
OFFSETS = (1, -1, BLOCK_ROW, -BLOCK_ROW, BLOCK_ROW - 1, 1 - BLOCK_ROW)
LANES = 128
CUTS = (1, 1, 1, 1)


def up(value, step):
    return -(-value // step) * step


def slots(length):
    side = CELLS_Y
    counts = (side, side, length, length, 1, 1)
    order = (2, 3, 0, 1, 4, 5)
    base = [0] * 6
    at = 0
    for k in order:
        base[k] = at
        at += up(counts[k], 8)
    return tuple(base), counts, at


def bounds(rows):
    parts = rows // LANES
    total = sum(CUTS)
    edges = [0]
    for k in range(len(CUTS)):
        edges.append(parts * sum(CUTS[: k + 1]) // total * LANES)
    return edges


def split(values):
    high = values.astype(jnp.bfloat16)
    low = (values - high.astype(jnp.float32)).astype(jnp.bfloat16)
    return high, low


def kernel(
    devices,
    field_hbm, dv_hbm, dc_hbm, ends_hbm, edges_hbm, send_hbm, area_hbm, level_hbm,
    out_ref,
    landed, flat, first, matrix, rim, pair, selector, outgoing, incoming, corner_out, corner_in,
    weight, packed, index, near_ref, coef_ref,
    dv_ref, dc_ref, ends_ref, edges_ref, send_ref, area_ref, level_ref, scale_ref,
    load_sem, table_sem, send_sem, recv_sem,
):
    fields_n, levels_n, cell_count = field_hbm.shape
    stride = up(levels_n, 8)
    rows = flat.shape[0]
    cuts = bounds(rows)
    chunks = len(cuts) - 1
    halo = rim.shape[0] // 2
    length = send_ref.shape[1]
    edge_count = ends_ref.shape[1]
    base, counts, used = slots(length)
    me = lax.axis_index("cells")
    targets = [lax.rem(me + (o + devices), devices) for o in OFFSETS]
    tiles = cell_count // LANES

    send_load = pltpu.make_async_copy(send_hbm, send_ref, table_sem.at[0])
    send_load.start()
    loads = [
        pltpu.make_async_copy(field_hbm.at[f], landed.at[f], load_sem.at[f])
        for f in range(fields_n)
    ]
    for load in loads:
        load.start()
    pairs = (
        (dv_hbm, dv_ref), (dc_hbm, dc_ref), (ends_hbm, ends_ref), (edges_hbm, edges_ref),
        (area_hbm, area_ref), (level_hbm, level_ref),
    )
    tables = [
        pltpu.make_async_copy(a, b, table_sem.at[i + 1]) for i, (a, b) in enumerate(pairs)
    ]
    for load in tables:
        load.start()

    barrier = pltpu.get_barrier_semaphore()
    for target in targets:
        pl.semaphore_signal(
            barrier, inc=1, device_id=(target,), device_id_type=pl.DeviceIdType.MESH
        )

    send_load.wait()
    for k in range(6):
        height = up(counts[k], 8)
        r = lax.broadcasted_iota(jnp.int32, (height, length), 0)
        c = lax.broadcasted_iota(jnp.int32, (height, length), 1)
        ids = send_ref[k : k + 1, :].astype(jnp.float32)
        column = jnp.sum(jnp.where(r == c, ids, 0.0), axis=1, keepdims=True)
        column = jnp.broadcast_to(column, (height, LANES)).astype(jnp.int32)
        lane = lax.broadcasted_iota(jnp.int32, (height, LANES), 1)
        for tile in range(tiles):
            hit = column == lane + tile * LANES
            ones = jnp.where(hit, 1.0, 0.0).astype(jnp.bfloat16)
            selector[base[k] : base[k] + height, tile * LANES : (tile + 1) * LANES] = ones

    def spread(values, c):
        low_at = cuts[c + 1] - cuts[c]
        high, low = split(values)
        pair[2 * cuts[c] : 2 * cuts[c] + low_at, :] = high
        pair[2 * cuts[c] + low_at : 2 * cuts[c + 1], :] = low

    def copies(lap, c):
        here = pl.ds(cuts[c], cuts[c + 1] - cuts[c])

        def ends(k):
            if k < 4:
                some = pl.ds(base[k], counts[k])
                return outgoing.at[lap, some, here], incoming.at[lap, some, here]
            return corner_out.at[lap, k - 4, :, here], corner_in.at[lap, k - 4, :, here]

        return [
            pltpu.make_async_remote_copy(
                src_ref=ends(k)[0],
                dst_ref=ends(k)[1],
                send_sem=send_sem.at[lap, c, k],
                recv_sem=recv_sem.at[lap, c, k],
                device_id=(targets[k],),
                device_id_type=pl.DeviceIdType.MESH,
            )
            for k in (2, 3, 4, 5, 0, 1)
        ]

    def send(lap, c):
        size = cuts[c + 1] - cuts[c]
        both = lax.dot_general(
            selector[...],
            pair[2 * cuts[c] : 2 * cuts[c + 1], :],
            (((1,), (1,)), ((), ())),
            preferred_element_type=jnp.float32,
        )
        here = slice(cuts[c], cuts[c + 1])
        both = both[:, :size] + both[:, size:]
        outgoing[lap, :, here] = both[: base[4]]
        for k in (4, 5):
            corner_out[lap, k - 4, :, here] = both[base[k] : base[k] + 1]
        for copy in copies(lap, c):
            copy.start()

    def own(c):
        size = cuts[c + 1] - cuts[c]
        at = 2 * cuts[c]
        both = jnp.dot(
            pair[at : at + 2 * size, :],
            matrix[:cell_count, :],
            preferred_element_type=jnp.float32,
        )
        fine = jnp.dot(
            pair[at : at + size, :],
            matrix[cell_count:, :],
            preferred_element_type=jnp.float32,
        )
        return both[:size] + both[size:] + fine

    def outside(lap, c):
        size = cuts[c + 1] - cuts[c]
        here = slice(cuts[c], cuts[c + 1])
        for copy in copies(lap, c):
            copy.wait_recv()
        corners = jnp.zeros((halo - base[4], size), jnp.float32)
        place = lax.broadcasted_iota(jnp.int32, corners.shape, 0)
        for k in (4, 5):
            value = jnp.broadcast_to(corner_in[lap, k - 4, :, here], corners.shape)
            corners = jnp.where(place == base[k] - base[4], value, corners)
        whole = jnp.concatenate([incoming[lap, :, here], corners], axis=0)
        high, low = split(whole.T)
        lhs = jnp.concatenate([high, low], axis=0)
        both = jnp.dot(lhs, rim[:halo, :], preferred_element_type=jnp.float32)
        fine = jnp.dot(high, rim[halo:, :], preferred_element_type=jnp.float32)
        return both[:size] + both[size:] + fine

    loaded = 0
    for c in range(chunks):
        need = min(fields_n, -(-cuts[c + 1] // stride))
        for f in range(loaded, need):
            loads[f].wait()
            flat[f * stride : f * stride + levels_n, :] = landed[f]
        loaded = max(loaded, need)
        spread(flat[cuts[c] : cuts[c + 1], :], c)
        if c == 0:
            pl.semaphore_wait(barrier, len(targets))
        send(0, c)

    for load in tables:
        load.wait()
    edge_tiles = weight.shape[1] // LANES
    weight[...] = jnp.zeros_like(weight)
    packed[...] = jnp.zeros_like(packed)
    index[...] = jnp.zeros_like(index)
    for k in range(edge_tiles):
        part = slice(k * LANES, min((k + 1) * LANES, edge_count))
        weight[0, part] = dv_ref[part] / dc_ref[part]
    packed[:, :edge_count] = ends_ref[0:1, :] + ends_ref[1:2, :] * 4096
    index[0:6, :] = edges_ref[...]
    row = lax.broadcasted_iota(jnp.int32, (8, LANES), 0)
    lane = lax.broadcasted_iota(jnp.int32, (8, LANES), 1)
    for tile in range(tiles):
        here = slice(tile * LANES, (tile + 1) * LANES)
        wanted = index[:, here]
        high = wanted >> 7
        low = wanted & 127
        w = jnp.zeros((8, LANES), jnp.float32)
        p = jnp.zeros((8, LANES), jnp.int32)
        for k in range(edge_tiles):
            part = slice(k * LANES, (k + 1) * LANES)
            wk = jnp.broadcast_to(weight[0:1, part], (8, LANES))
            pk = jnp.broadcast_to(packed[0:1, part], (8, LANES))
            hit = high == k
            w = jnp.where(hit, jnp.take_along_axis(wk, low, axis=1), w)
            p = jnp.where(hit, jnp.take_along_axis(pk, low, axis=1), p)
        lower = p & 4095
        upper = p >> 12
        other = jnp.where(lower == lane + tile * LANES, upper, lower)
        away = other - cell_count
        place = jnp.zeros((8, LANES), jnp.int32)
        for k in range(6):
            inside = (away >= k * length) & (away < (k + 1) * length)
            place = jnp.where(inside, away - k * length + base[k], place)
        near = jnp.where(away < 0, other, cell_count + place)
        share = w / jnp.broadcast_to(area_ref[here], (8, LANES))
        share = jnp.where(row < 6, share, 0.0)
        total = jnp.sum(share, axis=0, keepdims=True)
        near_ref[:, here] = jnp.where(row < 6, near, -1)
        coef_ref[:, here] = jnp.where(row == 6, total, share)
    r = lax.broadcasted_iota(jnp.int32, (stride, levels_n), 0)
    c = lax.broadcasted_iota(jnp.int32, (stride, levels_n), 1)
    levels = jnp.broadcast_to(level_ref[...].reshape(1, levels_n), (stride, levels_n))
    column = jnp.sum(jnp.where(r == c, -levels, 0.0), axis=1, keepdims=True)
    scale_ref[...] = jnp.broadcast_to(column, (stride, LANES))

    ids = lax.broadcasted_iota(jnp.int32, (LANES, LANES), 0)

    def entries(start, tile):
        here = slice(tile * LANES, (tile + 1) * LANES)
        block = jnp.zeros((LANES, LANES), jnp.float32)
        for j in range(6):
            hit = ids == near_ref[j : j + 1, here] - start
            block = jnp.where(hit, coef_ref[j : j + 1, here], block)
        return split(block)

    def fill(r, carry):
        start = pl.multiple_of(r * LANES, LANES)
        for tile in range(tiles):
            here = slice(tile * LANES, (tile + 1) * LANES)
            high, low = entries(start, tile)
            matrix[pl.ds(start, LANES), here] = high
            matrix[pl.ds(start + cell_count, LANES), here] = low
        return carry

    lax.fori_loop(0, tiles, fill, 0)
    for r in range(halo // LANES):
        for tile in range(tiles):
            here = slice(tile * LANES, (tile + 1) * LANES)
            high, low = entries(cell_count + r * LANES, tile)
            rim[r * LANES : (r + 1) * LANES, here] = high
            rim[halo + r * LANES : halo + (r + 1) * LANES, here] = low

    for c in range(chunks):
        part = slice(cuts[c], cuts[c + 1])
        first[part, :] = own(c) - flat[part, :] * coef_ref[6:7, :]
        result = first[part, :] + outside(0, c)
        first[part, :] = result
        spread(result, c)
        send(1, c)
    for c in range(chunks):
        part = slice(cuts[c], cuts[c + 1])
        flat[part, :] = own(c) - first[part, :] * coef_ref[6:7, :]
    for c in range(chunks):
        part = slice(cuts[c], cuts[c + 1])
        flat[part, :] = flat[part, :] + outside(1, c)
        for f in range(fields_n):
            lo = max(cuts[c], f * stride)
            hi = min(cuts[c + 1], (f + 1) * stride)
            if lo >= hi:
                continue
            at = lo - f * stride
            size = min(hi - f * stride, levels_n) - at
            scale = jnp.broadcast_to(scale_ref[at : at + size, 0:1], (size, cell_count))
            out_ref[f, at : at + size, :] = flat[lo : lo + size, :] * scale
    for lap in range(2):
        for c in range(chunks):
            for copy in copies(lap, c):
                copy.wait_send()


def shards(
    devices, field, cell_area, dv_edge, dc_edge, cells_on_edge, edges_on_cell, send_cells,
    level_coef,
):
    length = send_cells.shape[1]
    fields_n, levels_n, cell_count = field.shape
    edge_count = dv_edge.shape[0]
    base, _, used = slots(length)
    halo = up(used, LANES)
    stride = up(levels_n, 8)
    rows = up(fields_n * stride, LANES)
    chunks = len(bounds(rows)) - 1
    vmem = pl.BlockSpec(memory_space=pltpu.VMEM)
    hbm = pl.BlockSpec(memory_space=pltpu.HBM)
    return pl.pallas_call(
        functools.partial(kernel, devices),
        out_shape=pltpu.VMEM(field.shape, jnp.float32),
        in_specs=[hbm] * 8,
        out_specs=vmem,
        scratch_shapes=[
            pltpu.VMEM(field.shape, jnp.float32),
            pltpu.VMEM((rows, cell_count), jnp.float32),
            pltpu.VMEM((rows, cell_count), jnp.float32),
            pltpu.VMEM((2 * cell_count, cell_count), jnp.bfloat16),
            pltpu.VMEM((2 * halo, cell_count), jnp.bfloat16),
            pltpu.VMEM((2 * rows, cell_count), jnp.bfloat16),
            pltpu.VMEM((used, cell_count), jnp.bfloat16),
            pltpu.VMEM((2, base[4], rows), jnp.float32),
            pltpu.VMEM((2, base[4], rows), jnp.float32),
            pltpu.VMEM((2, 2, 1, rows), jnp.float32),
            pltpu.VMEM((2, 2, 1, rows), jnp.float32),
            pltpu.VMEM((1, up(edge_count, LANES)), jnp.float32),
            pltpu.VMEM((1, up(edge_count, LANES)), jnp.int32),
            pltpu.VMEM((8, cell_count), jnp.int32),
            pltpu.VMEM((8, cell_count), jnp.int32),
            pltpu.VMEM((8, cell_count), jnp.float32),
            pltpu.VMEM(dv_edge.shape, jnp.float32),
            pltpu.VMEM(dc_edge.shape, jnp.float32),
            pltpu.VMEM(cells_on_edge.shape, jnp.int32),
            pltpu.VMEM(edges_on_cell.shape, jnp.int32),
            pltpu.VMEM(send_cells.shape, jnp.int32),
            pltpu.VMEM(cell_area.shape, jnp.float32),
            pltpu.VMEM(level_coef.shape, jnp.float32),
            pltpu.VMEM((stride, LANES), jnp.float32),
            pltpu.SemaphoreType.DMA((fields_n,)),
            pltpu.SemaphoreType.DMA((7,)),
            pltpu.SemaphoreType.DMA((2, chunks, 6)),
            pltpu.SemaphoreType.DMA((2, chunks, 6)),
        ],
        compiler_params=pltpu.CompilerParams(
            collective_id=0,
            has_side_effects=True,
            vmem_limit_bytes=67043328 - up(fields_n * stride * cell_count * 4, 1024),
        ),
        name="diffuse",
    )(
        field, dv_edge, dc_edge, cells_on_edge, edges_on_cell, send_cells, cell_area, level_coef
    )


def solution(mesh):
    return jax.shard_map(
        functools.partial(shards, mesh.shape["cells"]),
        mesh=mesh,
        in_specs=(
            P(None, None, "cells"),
            P("cells"),
            P("cells"),
            P("cells"),
            P(None, "cells"),
            P(None, "cells"),
            P(None, "cells"),
            P(),
        ),
        out_specs=P(None, None, "cells"),
        check_vma=False,
    )
```

```python
import functools

import jax
import jax.numpy as jnp
from jax import lax
from jax.experimental import pallas as pl
from jax.experimental.pallas import tpu as pltpu
from jax.sharding import PartitionSpec as P

CELLS_Y = 16
BLOCK_ROW = 16
OFFSETS = (1, -1, BLOCK_ROW, -BLOCK_ROW, BLOCK_ROW - 1, 1 - BLOCK_ROW)
LANES = 128
UNIT = 16
CUTS = (8, 8, 8, 7)
ORDER = ((1, 0), (1, 1), (1, 2), (1, 3), (0, 0), (0, 1), (0, 2), (0, 3), (2, 0), (2, 1), (2, 2), (2, 3))


def up(value, step):
    return -(-value // step) * step


def slots(length):
    side = CELLS_Y
    counts = (side, side, length, length, 1, 1)
    order = (2, 3, 0, 1, 4, 5)
    base = [0] * 6
    at = 0
    for k in order:
        base[k] = at
        at += counts[k]
    return tuple(base), counts, at


def layout(fields_n, levels_n):
    stride = up(levels_n, 8)
    whole = levels_n // 8 * 8
    rest = levels_n - whole
    gaps = [
        f * stride + l for f in range(fields_n - 1) for l in range(levels_n, stride)
    ]
    last = (fields_n - 1) * stride
    parts = [(f, 0, levels_n, f * stride) for f in range(fields_n - 1)]
    if rest <= len(gaps) and (last + whole) % UNIT == 0:
        parts.append((fields_n - 1, 0, whole, last))
        parts += [(fields_n - 1, whole + i, 1, gaps[i]) for i in range(rest)]
        return parts, gaps[rest:], last + whole
    parts.append((fields_n - 1, 0, levels_n, last))
    rows = up(last + levels_n, UNIT)
    return parts, gaps + list(range(last + levels_n, rows)), rows


def bounds(rows):
    parts = rows // UNIT
    total = sum(CUTS)
    return [parts * sum(CUTS[:k]) // total * UNIT for k in range(len(CUTS) + 1)]


def split(values):
    high = values.astype(jnp.bfloat16)
    low = (values - high.astype(jnp.float32)).astype(jnp.bfloat16)
    return high, low


def kernel(
    devices,
    field_hbm, dv_hbm, dc_hbm, ends_hbm, edges_hbm, send_hbm, area_hbm, level_hbm,
    out_ref,
    landed, flat, first, matrix, rim, pair, selector, rim_out, rim_in, side_out, side_in,
    corner_out, corner_in, lists, weight, packed, index, near_ref, coef_ref,
    dv_ref, dc_ref, ends_ref, edges_ref, send_ref, area_ref, level_ref, scale_ref,
    load_sem, table_sem, send_sem, recv_sem,
):
    fields_n, levels_n, cell_count = field_hbm.shape
    parts, gaps, rows = layout(fields_n, levels_n)
    cuts = bounds(rows)
    chunks = len(cuts) - 1
    widths = [up(cuts[c + 1] - cuts[c], LANES) for c in range(chunks)]
    starts = [sum(widths[:c]) for c in range(chunks)]
    halo = rim.shape[0] // 2
    length = send_ref.shape[1]
    edge_count = ends_ref.shape[1]
    base, counts, used = slots(length)
    me = lax.axis_index("cells")
    targets = [lax.rem(me + (o + devices), devices) for o in OFFSETS]
    tiles = cell_count // LANES

    barrier = pltpu.get_barrier_semaphore()
    for target in targets:
        pl.semaphore_signal(
            barrier, inc=1, device_id=(target,), device_id_type=pl.DeviceIdType.MESH
        )

    send_load = pltpu.make_async_copy(send_hbm, send_ref, table_sem.at[0])
    send_load.start()
    loads = [
        pltpu.make_async_copy(field_hbm.at[f], landed.at[f], load_sem.at[f])
        for f in range(fields_n)
    ]
    for load in loads:
        load.start()
    pairs = (
        (dv_hbm, dv_ref), (dc_hbm, dc_ref), (ends_hbm, ends_ref), (edges_hbm, edges_ref),
        (area_hbm, area_ref), (level_hbm, level_ref),
    )
    tables = [
        pltpu.make_async_copy(a, b, table_sem.at[i + 1]) for i, (a, b) in enumerate(pairs)
    ]
    for load in tables:
        load.start()

    send_load.wait()
    lists[0:6, 0:length] = send_ref[...]
    table = lists[...]
    lane = lax.broadcasted_iota(jnp.int32, (1, LANES), 1)
    picks = [jnp.full((1, LANES), -1, jnp.int32)] * (halo // LANES)
    for k in range(6):
        tile, at = base[k] // LANES, base[k] % LANES
        moved = pltpu.roll(table, at, 1) if at else table
        inside = (lane >= at) & (lane < at + counts[k])
        picks[tile] = jnp.where(inside, moved[k : k + 1], picks[tile])
    ids = lax.broadcasted_iota(jnp.int32, (LANES, LANES), 0)
    for r in range(tiles):
        for tile in range(halo // LANES):
            hit = ids == picks[tile] - r * LANES
            selector[r * LANES : (r + 1) * LANES, tile * LANES : (tile + 1) * LANES] = (
                jnp.where(hit, 1.0, 0.0).astype(jnp.bfloat16)
            )

    def spread(values, c):
        low_at = cuts[c + 1] - cuts[c]
        high, low = split(values)
        pair[2 * cuts[c] : 2 * cuts[c] + low_at, :] = high
        pair[2 * cuts[c] + low_at : 2 * cuts[c + 1], :] = low

    def copies(lap, c):
        half = pl.ds(cuts[c] // 2, (cuts[c + 1] - cuts[c]) // 2)
        here = pl.ds(starts[c], widths[c])

        def ends(k):
            if k in (2, 3):
                return rim_out.at[lap, k - 2, half], rim_in.at[lap, k - 2, half]
            if k in (0, 1):
                return side_out.at[lap, k, :, here], side_in.at[lap, k, :, here]
            return corner_out.at[lap, k - 4, :, here], corner_in.at[lap, k - 4, :, here]

        return [
            pltpu.make_async_remote_copy(
                src_ref=ends(k)[0],
                dst_ref=ends(k)[1],
                send_sem=send_sem.at[lap, c, k],
                recv_sem=recv_sem.at[lap, c, k],
                device_id=(targets[k],),
                device_id_type=pl.DeviceIdType.MESH,
            )
            for k in (4, 5, 0, 1, 2, 3)
        ]

    def send(lap, c):
        size = cuts[c + 1] - cuts[c]
        h = size // 2
        both = jnp.dot(
            pair[2 * cuts[c] : 2 * cuts[c + 1], :],
            selector[...],
            preferred_element_type=jnp.float32,
        )
        both = both[:size] + both[size:]
        edge = both[:, :LANES]
        turned = pltpu.roll(edge, length, 1)
        left = lax.broadcasted_iota(jnp.int32, (h, LANES), 1) < length
        half = slice(cuts[c] // 2, cuts[c + 1] // 2)
        rim_out[lap, 0, half, :] = jnp.where(left, edge[:h], turned[h:])
        rim_out[lap, 1, half, :] = jnp.where(left, turned[:h], edge[h:])
        small = both[:, LANES:]
        if size < widths[c]:
            fill = jnp.zeros((widths[c] - size, LANES), jnp.float32)
            small = jnp.concatenate([small, fill], axis=0)
        small = small.T
        here = slice(starts[c], starts[c] + widths[c])
        for k in (0, 1):
            at = base[k] - LANES
            side_out[lap, k, :, here] = small[at : at + counts[k]]
        for k in (4, 5):
            at = base[k] - LANES
            corner_out[lap, k - 4, :, here] = small[at : at + 1]
        for copy in copies(lap, c):
            copy.start()

    def own(c):
        size = cuts[c + 1] - cuts[c]
        at = 2 * cuts[c]
        both = jnp.dot(
            pair[at : at + 2 * size, :],
            matrix[:cell_count, :],
            preferred_element_type=jnp.float32,
        )
        fine = jnp.dot(
            pair[at : at + size, :],
            matrix[cell_count:, :],
            preferred_element_type=jnp.float32,
        )
        return both[:size] + both[size:] + fine

    def outside(lap, c):
        size = cuts[c + 1] - cuts[c]
        h = size // 2
        for copy in copies(lap, c):
            copy.wait_recv()
        half = slice(cuts[c] // 2, cuts[c + 1] // 2)
        here = slice(starts[c], starts[c] + widths[c])
        left = lax.broadcasted_iota(jnp.int32, (h, LANES), 1) < length
        above = rim_in[lap, 0, half, :]
        below = rim_in[lap, 1, half, :]
        edge = jnp.concatenate(
            [
                jnp.where(left, above, pltpu.roll(below, length, 1)),
                jnp.where(left, pltpu.roll(above, length, 1), below),
            ],
            axis=0,
        )
        ends = base[4] - LANES
        corners = jnp.zeros((LANES - ends, widths[c]), jnp.float32)
        place = lax.broadcasted_iota(jnp.int32, corners.shape, 0)
        for k in (4, 5):
            value = jnp.broadcast_to(corner_in[lap, k - 4, :, here], corners.shape)
            corners = jnp.where(place == base[k] - base[4], value, corners)
        small = jnp.concatenate(
            [side_in[lap, 0, :, here], side_in[lap, 1, :, here], corners], axis=0
        )
        high, low = split(jnp.concatenate([edge, small.T[:size]], axis=1))
        lhs = jnp.concatenate([high, low], axis=0)
        both = jnp.dot(lhs, rim[:halo, :], preferred_element_type=jnp.float32)
        fine = jnp.dot(high, rim[halo:, :], preferred_element_type=jnp.float32)
        return both[:size] + both[size:] + fine

    for row in gaps:
        flat[row : row + 1, :] = jnp.zeros((1, cell_count), jnp.float32)
    loaded = set()
    for c in range(chunks):
        need = {f for f, _, _, row in parts if row < cuts[c + 1]}
        for f in sorted(need - loaded):
            loads[f].wait()
            for g, level, size, row in parts:
                if g == f:
                    flat[row : row + size, :] = landed[f, level : level + size, :]
        loaded |= need
        spread(flat[cuts[c] : cuts[c + 1], :], c)
        if c == 0:
            pl.semaphore_wait(barrier, len(targets))
        send(0, c)

    for load in tables:
        load.wait()
    edge_tiles = weight.shape[1] // LANES
    weight[...] = jnp.zeros_like(weight)
    packed[...] = jnp.zeros_like(packed)
    index[...] = jnp.zeros_like(index)
    for k in range(edge_tiles):
        part = slice(k * LANES, min((k + 1) * LANES, edge_count))
        weight[0, part] = dv_ref[part] / dc_ref[part]
    packed[:, :edge_count] = ends_ref[0:1, :] + ends_ref[1:2, :] * 4096
    index[0:6, :] = edges_ref[...]
    row = lax.broadcasted_iota(jnp.int32, (8, LANES), 0)
    lane = lax.broadcasted_iota(jnp.int32, (8, LANES), 1)
    for tile in range(tiles):
        here = slice(tile * LANES, (tile + 1) * LANES)
        wanted = index[:, here]
        high = wanted >> 7
        low = wanted & 127
        w = jnp.zeros((8, LANES), jnp.float32)
        p = jnp.zeros((8, LANES), jnp.int32)
        for k in range(edge_tiles):
            part = slice(k * LANES, (k + 1) * LANES)
            wk = jnp.broadcast_to(weight[0:1, part], (8, LANES))
            pk = jnp.broadcast_to(packed[0:1, part], (8, LANES))
            hit = high == k
            w = jnp.where(hit, jnp.take_along_axis(wk, low, axis=1), w)
            p = jnp.where(hit, jnp.take_along_axis(pk, low, axis=1), p)
        lower = p & 4095
        upper = p >> 12
        other = jnp.where(lower == lane + tile * LANES, upper, lower)
        away = other - cell_count
        place = jnp.zeros((8, LANES), jnp.int32)
        for k in range(6):
            inside = (away >= k * length) & (away < (k + 1) * length)
            place = jnp.where(inside, away - k * length + base[k], place)
        near = jnp.where(away < 0, other, cell_count + place)
        share = w / jnp.broadcast_to(area_ref[here], (8, LANES))
        share = jnp.where(row < 6, share, 0.0)
        total = jnp.sum(share, axis=0, keepdims=True)
        near_ref[:, here] = jnp.where(row < 6, near, -1)
        coef_ref[:, here] = jnp.where(row == 6, total, share)
    tall = scale_ref.shape[0]
    r = lax.broadcasted_iota(jnp.int32, (tall, levels_n), 0)
    c = lax.broadcasted_iota(jnp.int32, (tall, levels_n), 1)
    levels = jnp.broadcast_to(level_ref[...].reshape(1, levels_n), (tall, levels_n))
    column = jnp.sum(jnp.where(r == c, -levels, 0.0), axis=1, keepdims=True)
    scale_ref[...] = jnp.broadcast_to(column, (tall, LANES))

    def entries(start, tile):
        here = slice(tile * LANES, (tile + 1) * LANES)
        block = jnp.zeros((LANES, LANES), jnp.float32)
        for j in range(6):
            hit = ids == near_ref[j : j + 1, here] - start
            block = jnp.where(hit, coef_ref[j : j + 1, here], block)
        return split(block)

    def fill(r, carry):
        start = pl.multiple_of(r * LANES, LANES)
        for tile in range(tiles):
            here = slice(tile * LANES, (tile + 1) * LANES)
            high, low = entries(start, tile)
            matrix[pl.ds(start, LANES), here] = high
            matrix[pl.ds(start + cell_count, LANES), here] = low
        return carry

    lax.fori_loop(0, tiles, fill, 0)
    for r in range(halo // LANES):
        for tile in range(tiles):
            here = slice(tile * LANES, (tile + 1) * LANES)
            high, low = entries(cell_count + r * LANES, tile)
            rim[r * LANES : (r + 1) * LANES, here] = high
            rim[halo + r * LANES : halo + (r + 1) * LANES, here] = low

    def relay(c):
        part = slice(cuts[c], cuts[c + 1])
        first[part, :] = own(c) - flat[part, :] * coef_ref[6:7, :]
        result = first[part, :] + outside(0, c)
        first[part, :] = result
        spread(result, c)
        send(1, c)

    def inner(c):
        part = slice(cuts[c], cuts[c + 1])
        flat[part, :] = own(c) - first[part, :] * coef_ref[6:7, :]

    def finish(c):
        part = slice(cuts[c], cuts[c + 1])
        flat[part, :] = flat[part, :] + outside(1, c)
        for f, level, size, row in parts:
            lo = max(cuts[c], row)
            hi = min(cuts[c + 1], row + size)
            if lo >= hi:
                continue
            at = level + lo - row
            scale = jnp.broadcast_to(scale_ref[at : at + hi - lo, 0:1], (hi - lo, cell_count))
            out_ref[f, at : at + hi - lo, :] = flat[lo:hi, :] * scale

    for step, c in ORDER:
        (inner, relay, finish)[step](c)
    for lap in range(2):
        for c in range(chunks):
            for copy in copies(lap, c):
                copy.wait_send()


def shards(
    devices, field, cell_area, dv_edge, dc_edge, cells_on_edge, edges_on_cell, send_cells,
    level_coef,
):
    length = send_cells.shape[1]
    fields_n, levels_n, cell_count = field.shape
    edge_count = dv_edge.shape[0]
    _, _, used = slots(length)
    halo = up(used, LANES)
    _, _, rows = layout(fields_n, levels_n)
    cuts = bounds(rows)
    chunks = len(cuts) - 1
    wide = sum(up(cuts[c + 1] - cuts[c], LANES) for c in range(chunks))
    vmem = pl.BlockSpec(memory_space=pltpu.VMEM)
    hbm = pl.BlockSpec(memory_space=pltpu.HBM)
    return pl.pallas_call(
        functools.partial(kernel, devices),
        out_shape=pltpu.VMEM(field.shape, jnp.float32),
        in_specs=[hbm] * 8,
        out_specs=vmem,
        scratch_shapes=[
            pltpu.VMEM(field.shape, jnp.float32),
            pltpu.VMEM((rows, cell_count), jnp.float32),
            pltpu.VMEM((rows, cell_count), jnp.float32),
            pltpu.VMEM((2 * cell_count, cell_count), jnp.bfloat16),
            pltpu.VMEM((2 * halo, cell_count), jnp.bfloat16),
            pltpu.VMEM((2 * rows, cell_count), jnp.bfloat16),
            pltpu.VMEM((cell_count, halo), jnp.bfloat16),
            pltpu.VMEM((2, 2, rows // 2, 2 * length), jnp.float32),
            pltpu.VMEM((2, 2, rows // 2, 2 * length), jnp.float32),
            pltpu.VMEM((2, 2, CELLS_Y, wide), jnp.float32),
            pltpu.VMEM((2, 2, CELLS_Y, wide), jnp.float32),
            pltpu.VMEM((2, 2, 1, wide), jnp.float32),
            pltpu.VMEM((2, 2, 1, wide), jnp.float32),
            pltpu.VMEM((8, LANES), jnp.int32),
            pltpu.VMEM((1, up(edge_count, LANES)), jnp.float32),
            pltpu.VMEM((1, up(edge_count, LANES)), jnp.int32),
            pltpu.VMEM((8, cell_count), jnp.int32),
            pltpu.VMEM((8, cell_count), jnp.int32),
            pltpu.VMEM((8, cell_count), jnp.float32),
            pltpu.VMEM(dv_edge.shape, jnp.float32),
            pltpu.VMEM(dc_edge.shape, jnp.float32),
            pltpu.VMEM(cells_on_edge.shape, jnp.int32),
            pltpu.VMEM(edges_on_cell.shape, jnp.int32),
            pltpu.VMEM(send_cells.shape, jnp.int32),
            pltpu.VMEM(cell_area.shape, jnp.float32),
            pltpu.VMEM(level_coef.shape, jnp.float32),
            pltpu.VMEM((up(levels_n, 8), LANES), jnp.float32),
            pltpu.SemaphoreType.DMA((fields_n,)),
            pltpu.SemaphoreType.DMA((7,)),
            pltpu.SemaphoreType.DMA((2, chunks, 6)),
            pltpu.SemaphoreType.DMA((2, chunks, 6)),
        ],
        compiler_params=pltpu.CompilerParams(
            collective_id=0,
            has_side_effects=True,
            vmem_limit_bytes=67043328 - fields_n * up(levels_n, 8) * cell_count * 4,
        ),
        name="diffuse",
    )(
        field, dv_edge, dc_edge, cells_on_edge, edges_on_cell, send_cells, cell_area, level_coef
    )


def solution(mesh):
    return jax.shard_map(
        functools.partial(shards, mesh.shape["cells"]),
        mesh=mesh,
        in_specs=(
            P(None, None, "cells"),
            P("cells"),
            P("cells"),
            P("cells"),
            P(None, "cells"),
            P(None, "cells"),
            P(None, "cells"),
            P(),
        ),
        out_specs=P(None, None, "cells"),
        check_vma=False,
    )
```

```python
import functools

import jax
import jax.numpy as jnp
from jax import lax
from jax.experimental import pallas as pl
from jax.experimental.pallas import tpu as pltpu
from jax.sharding import PartitionSpec as P

CELLS_Y = 16
BLOCK_ROW = 16
OFFSETS = (1, -1, BLOCK_ROW, -BLOCK_ROW, BLOCK_ROW - 1, 1 - BLOCK_ROW)
LANES = 128
UNIT = 16
CUTS = (8, 8, 8, 7)
ORDER = ((1, 0), (1, 1), (1, 2), (1, 3), (0, 0), (0, 1), (0, 2), (0, 3), (2, 0), (2, 1), (2, 2), (2, 3))


def up(value, step):
    return -(-value // step) * step


def slots(length):
    side = CELLS_Y
    counts = (side, side, length, length, 1, 1)
    order = (2, 3, 0, 1, 4, 5)
    base = [0] * 6
    at = 0
    for k in order:
        base[k] = at
        at += counts[k]
    return tuple(base), counts, at


def layout(fields_n, levels_n):
    stride = up(levels_n, 8)
    whole = levels_n // 8 * 8
    rest = levels_n - whole
    gaps = [
        f * stride + l for f in range(fields_n - 1) for l in range(levels_n, stride)
    ]
    last = (fields_n - 1) * stride
    parts = [(f, 0, levels_n, f * stride) for f in range(fields_n - 1)]
    if rest <= len(gaps) and (last + whole) % UNIT == 0:
        parts.append((fields_n - 1, 0, whole, last))
        parts += [(fields_n - 1, whole + i, 1, gaps[i]) for i in range(rest)]
        return parts, gaps[rest:], last + whole
    parts.append((fields_n - 1, 0, levels_n, last))
    rows = up(last + levels_n, UNIT)
    return parts, gaps + list(range(last + levels_n, rows)), rows


def bounds(rows):
    parts = rows // UNIT
    total = sum(CUTS)
    return [parts * sum(CUTS[:k]) // total * UNIT for k in range(len(CUTS) + 1)]


def gather(parts, cuts):
    groups = []
    for f in range(1 + max(part[0] for part in parts)):
        row = min(part[3] for part in parts if part[0] == f)
        c = max(k for k in range(len(cuts)) if cuts[k] <= row)
        if groups and groups[-1][2] == c:
            groups[-1][1] += 1
        else:
            groups.append([f, 1, c])
    return sorted(groups, key=lambda group: group[2])


def strips(cuts):
    starts = [0]
    for c in range(len(cuts) - 1):
        assert cuts[c + 1] - cuts[c] <= LANES
        starts.append(starts[-1] + cuts[c + 1] - cuts[c] + 2 * CELLS_Y)
    return starts


def split(values):
    high = values.astype(jnp.bfloat16)
    low = (values - high.astype(jnp.float32)).astype(jnp.bfloat16)
    return high, low


def kernel(
    devices,
    field_hbm, dv_hbm, dc_hbm, ends_hbm, edges_hbm, send_hbm, area_hbm, level_hbm,
    out_ref,
    landed, flat, first, matrix, rim, pair, selector, strip_out, strip_in,
    corner_out, corner_in, lists, weight, packed, index, near_ref, coef_ref,
    dv_ref, dc_ref, ends_ref, edges_ref, send_ref, area_ref, level_ref, scale_ref,
    load_sem, table_sem, send_sem, recv_sem,
):
    fields_n, levels_n, cell_count = field_hbm.shape
    parts, gaps, rows = layout(fields_n, levels_n)
    cuts = bounds(rows)
    chunks = len(cuts) - 1
    starts = strips(cuts)
    halo = rim.shape[0] // 2
    length = send_ref.shape[1]
    edge_count = ends_ref.shape[1]
    base, counts, used = slots(length)
    me = lax.axis_index("cells")
    targets = [lax.rem(me + (o + devices), devices) for o in OFFSETS]
    tiles = cell_count // LANES

    barrier = pltpu.get_barrier_semaphore()
    for target in targets:
        pl.semaphore_signal(
            barrier, inc=1, device_id=(target,), device_id_type=pl.DeviceIdType.MESH
        )

    send_load = pltpu.make_async_copy(send_hbm, send_ref, table_sem.at[0])
    send_load.start()
    groups = gather(parts, cuts)
    loads = [
        pltpu.make_async_copy(
            field_hbm.at[pl.ds(f, n)], landed.at[pl.ds(f, n)], load_sem.at[i]
        )
        for i, (f, n, _) in enumerate(groups)
    ]
    for load in loads:
        load.start()
    pairs = (
        (dv_hbm, dv_ref), (dc_hbm, dc_ref), (ends_hbm, ends_ref), (edges_hbm, edges_ref),
        (area_hbm, area_ref), (level_hbm, level_ref),
    )
    tables = [
        pltpu.make_async_copy(a, b, table_sem.at[i + 1]) for i, (a, b) in enumerate(pairs)
    ]
    for load in tables:
        load.start()

    send_load.wait()
    lists[0:6, 0:length] = send_ref[...]
    table = lists[...]
    lane = lax.broadcasted_iota(jnp.int32, (1, LANES), 1)
    picks = [jnp.full((1, LANES), -1, jnp.int32)] * (halo // LANES)
    for k in range(6):
        tile, at = base[k] // LANES, base[k] % LANES
        moved = pltpu.roll(table, at, 1) if at else table
        inside = (lane >= at) & (lane < at + counts[k])
        picks[tile] = jnp.where(inside, moved[k : k + 1], picks[tile])
    ids = lax.broadcasted_iota(jnp.int32, (LANES, LANES), 0)
    for r in range(tiles):
        for tile in range(halo // LANES):
            hit = ids == picks[tile] - r * LANES
            selector[r * LANES : (r + 1) * LANES, tile * LANES : (tile + 1) * LANES] = (
                jnp.where(hit, 1.0, 0.0).astype(jnp.bfloat16)
            )

    def spread(values, c):
        low_at = cuts[c + 1] - cuts[c]
        high, low = split(values)
        pair[2 * cuts[c] : 2 * cuts[c] + low_at, :] = high
        pair[2 * cuts[c] + low_at : 2 * cuts[c + 1], :] = low

    def places(c):
        h = (cuts[c + 1] - cuts[c]) // 2
        at = starts[c]
        side = at + 2 * h
        return (
            pl.ds(side, CELLS_Y), pl.ds(side + CELLS_Y, CELLS_Y), pl.ds(at, h), pl.ds(at + h, h)
        )

    def copies(lap, c):
        def ends(k):
            if k < 4:
                here = places(c)[k]
                return strip_out.at[lap, here], strip_in.at[lap, here]
            return corner_out.at[lap, c, k - 4], corner_in.at[lap, c, k - 4]

        return [
            pltpu.make_async_remote_copy(
                src_ref=ends(k)[0],
                dst_ref=ends(k)[1],
                send_sem=send_sem.at[k // 4],
                recv_sem=recv_sem.at[lap, c, k // 4],
                device_id=(targets[k],),
                device_id_type=pl.DeviceIdType.MESH,
            )
            for k in (4, 5, 0, 1, 2, 3)
        ]

    def receive(lap, c):
        strip = strip_in.at[lap, pl.ds(starts[c], starts[c + 1] - starts[c])]
        pltpu.make_async_copy(strip, strip, recv_sem.at[lap, c, 0]).wait()
        corner = corner_in.at[lap, c]
        pltpu.make_async_copy(corner, corner, recv_sem.at[lap, c, 1]).wait()

    def send(lap, c):
        size = cuts[c + 1] - cuts[c]
        h = size // 2
        both = jnp.dot(
            pair[2 * cuts[c] : 2 * cuts[c + 1], :],
            selector[...],
            preferred_element_type=jnp.float32,
        )
        both = both[:size] + both[size:]
        edge = both[:, :LANES]
        turned = pltpu.roll(edge, length, 1)
        left = lax.broadcasted_iota(jnp.int32, (h, LANES), 1) < length
        where = places(c)
        strip_out[lap, where[2], :] = jnp.where(left, edge[:h], turned[h:])
        strip_out[lap, where[3], :] = jnp.where(left, turned[:h], edge[h:])
        small = both[:, LANES:]
        if size < LANES:
            fill = jnp.zeros((LANES - size, LANES), jnp.float32)
            small = jnp.concatenate([small, fill], axis=0)
        small = small.T
        for k in (0, 1):
            at = base[k] - LANES
            strip_out[lap, where[k], :] = small[at : at + counts[k]]
        for k in (4, 5):
            at = base[k] - LANES
            corner_out[lap, c, k - 4] = small[at : at + 1]
        for copy in copies(lap, c):
            copy.start()

    def own(c):
        size = cuts[c + 1] - cuts[c]
        at = 2 * cuts[c]
        both = jnp.dot(
            pair[at : at + 2 * size, :],
            matrix[:cell_count, :],
            preferred_element_type=jnp.float32,
        )
        fine = jnp.dot(
            pair[at : at + size, :],
            matrix[cell_count:, :],
            preferred_element_type=jnp.float32,
        )
        return both[:size] + both[size:] + fine

    def outside(lap, c):
        size = cuts[c + 1] - cuts[c]
        h = size // 2
        receive(lap, c)
        where = places(c)
        left = lax.broadcasted_iota(jnp.int32, (h, LANES), 1) < length
        above = strip_in[lap, where[2], :]
        below = strip_in[lap, where[3], :]
        edge = jnp.concatenate(
            [
                jnp.where(left, above, pltpu.roll(below, length, 1)),
                jnp.where(left, pltpu.roll(above, length, 1), below),
            ],
            axis=0,
        )
        ends = base[4] - LANES
        corners = jnp.zeros((LANES - ends, LANES), jnp.float32)
        place = lax.broadcasted_iota(jnp.int32, corners.shape, 0)
        for k in (4, 5):
            value = jnp.broadcast_to(corner_in[lap, c, k - 4], corners.shape)
            corners = jnp.where(place == base[k] - base[4], value, corners)
        small = jnp.concatenate(
            [strip_in[lap, where[0], :], strip_in[lap, where[1], :], corners], axis=0
        )
        high, low = split(jnp.concatenate([edge, small.T[:size]], axis=1))
        lhs = jnp.concatenate([high, low], axis=0)
        both = jnp.dot(lhs, rim[:halo, :], preferred_element_type=jnp.float32)
        fine = jnp.dot(high, rim[halo:, :], preferred_element_type=jnp.float32)
        return both[:size] + both[size:] + fine

    for row in gaps:
        flat[row : row + 1, :] = jnp.zeros((1, cell_count), jnp.float32)
    for c in range(chunks):
        for load, (f, n, first_use) in zip(loads, groups):
            if first_use != c:
                continue
            load.wait()
            for g, level, size, row in parts:
                if f <= g < f + n:
                    flat[row : row + size, :] = landed[g, level : level + size, :]
        spread(flat[cuts[c] : cuts[c + 1], :], c)
        if c == 0:
            pl.semaphore_wait(barrier, len(targets))
        send(0, c)

    for load in tables:
        load.wait()
    edge_tiles = weight.shape[1] // LANES
    weight[...] = jnp.zeros_like(weight)
    packed[...] = jnp.zeros_like(packed)
    index[...] = jnp.zeros_like(index)
    for k in range(edge_tiles):
        part = slice(k * LANES, min((k + 1) * LANES, edge_count))
        weight[0, part] = dv_ref[part] / dc_ref[part]
    packed[:, :edge_count] = ends_ref[0:1, :] + ends_ref[1:2, :] * 4096
    index[0:6, :] = edges_ref[...]
    row = lax.broadcasted_iota(jnp.int32, (8, LANES), 0)
    lane = lax.broadcasted_iota(jnp.int32, (8, LANES), 1)
    for tile in range(tiles):
        here = slice(tile * LANES, (tile + 1) * LANES)
        wanted = index[:, here]
        high = wanted >> 7
        low = wanted & 127
        w = jnp.zeros((8, LANES), jnp.float32)
        p = jnp.zeros((8, LANES), jnp.int32)
        for k in range(edge_tiles):
            part = slice(k * LANES, (k + 1) * LANES)
            wk = jnp.broadcast_to(weight[0:1, part], (8, LANES))
            pk = jnp.broadcast_to(packed[0:1, part], (8, LANES))
            hit = high == k
            w = jnp.where(hit, jnp.take_along_axis(wk, low, axis=1), w)
            p = jnp.where(hit, jnp.take_along_axis(pk, low, axis=1), p)
        lower = p & 4095
        upper = p >> 12
        other = jnp.where(lower == lane + tile * LANES, upper, lower)
        away = other - cell_count
        place = jnp.zeros((8, LANES), jnp.int32)
        for k in range(6):
            inside = (away >= k * length) & (away < (k + 1) * length)
            place = jnp.where(inside, away - k * length + base[k], place)
        near = jnp.where(away < 0, other, cell_count + place)
        share = w / jnp.broadcast_to(area_ref[here], (8, LANES))
        share = jnp.where(row < 6, share, 0.0)
        total = jnp.sum(share, axis=0, keepdims=True)
        near_ref[:, here] = jnp.where(row < 6, near, -1)
        coef_ref[:, here] = jnp.where(row == 6, total, share)
    tall = scale_ref.shape[0]
    r = lax.broadcasted_iota(jnp.int32, (tall, levels_n), 0)
    c = lax.broadcasted_iota(jnp.int32, (tall, levels_n), 1)
    levels = jnp.broadcast_to(level_ref[...].reshape(1, levels_n), (tall, levels_n))
    column = jnp.sum(jnp.where(r == c, -levels, 0.0), axis=1, keepdims=True)
    scale_ref[...] = jnp.broadcast_to(column, (tall, LANES))

    def entries(start, tile):
        here = slice(tile * LANES, (tile + 1) * LANES)
        block = jnp.zeros((LANES, LANES), jnp.float32)
        for j in range(6):
            hit = ids == near_ref[j : j + 1, here] - start
            block = jnp.where(hit, coef_ref[j : j + 1, here], block)
        return split(block)

    def fill(r, carry):
        start = pl.multiple_of(r * LANES, LANES)
        for tile in range(tiles):
            here = slice(tile * LANES, (tile + 1) * LANES)
            high, low = entries(start, tile)
            matrix[pl.ds(start, LANES), here] = high
            matrix[pl.ds(start + cell_count, LANES), here] = low
        return carry

    lax.fori_loop(0, tiles, fill, 0)
    for r in range(halo // LANES):
        for tile in range(tiles):
            here = slice(tile * LANES, (tile + 1) * LANES)
            high, low = entries(cell_count + r * LANES, tile)
            rim[r * LANES : (r + 1) * LANES, here] = high
            rim[halo + r * LANES : halo + (r + 1) * LANES, here] = low

    def relay(c):
        part = slice(cuts[c], cuts[c + 1])
        first[part, :] = own(c) - flat[part, :] * coef_ref[6:7, :]
        result = first[part, :] + outside(0, c)
        first[part, :] = result
        spread(result, c)
        send(1, c)

    def inner(c):
        part = slice(cuts[c], cuts[c + 1])
        flat[part, :] = own(c) - first[part, :] * coef_ref[6:7, :]

    def finish(c):
        part = slice(cuts[c], cuts[c + 1])
        flat[part, :] = flat[part, :] + outside(1, c)
        for f, level, size, row in parts:
            lo = max(cuts[c], row)
            hi = min(cuts[c + 1], row + size)
            if lo >= hi:
                continue
            at = level + lo - row
            scale = jnp.broadcast_to(scale_ref[at : at + hi - lo, 0:1], (hi - lo, cell_count))
            out_ref[f, at : at + hi - lo, :] = flat[lo:hi, :] * scale

    for step, c in ORDER:
        (inner, relay, finish)[step](c)
    pltpu.make_async_copy(strip_out, strip_out, send_sem.at[0]).wait()
    pltpu.make_async_copy(corner_out, corner_out, send_sem.at[1]).wait()


def shards(
    devices, field, cell_area, dv_edge, dc_edge, cells_on_edge, edges_on_cell, send_cells,
    level_coef,
):
    length = send_cells.shape[1]
    fields_n, levels_n, cell_count = field.shape
    edge_count = dv_edge.shape[0]
    _, _, used = slots(length)
    halo = up(used, LANES)
    parts, _, rows = layout(fields_n, levels_n)
    cuts = bounds(rows)
    chunks = len(cuts) - 1
    tall = strips(cuts)[-1]
    vmem = pl.BlockSpec(memory_space=pltpu.VMEM)
    hbm = pl.BlockSpec(memory_space=pltpu.HBM)
    return pl.pallas_call(
        functools.partial(kernel, devices),
        out_shape=pltpu.VMEM(field.shape, jnp.float32),
        in_specs=[hbm] * 8,
        out_specs=vmem,
        scratch_shapes=[
            pltpu.VMEM(field.shape, jnp.float32),
            pltpu.VMEM((rows, cell_count), jnp.float32),
            pltpu.VMEM((rows, cell_count), jnp.float32),
            pltpu.VMEM((2 * cell_count, cell_count), jnp.bfloat16),
            pltpu.VMEM((2 * halo, cell_count), jnp.bfloat16),
            pltpu.VMEM((2 * rows, cell_count), jnp.bfloat16),
            pltpu.VMEM((cell_count, halo), jnp.bfloat16),
            pltpu.VMEM((2, tall, LANES), jnp.float32),
            pltpu.VMEM((2, tall, LANES), jnp.float32),
            pltpu.VMEM((2, chunks, 2, 1, LANES), jnp.float32),
            pltpu.VMEM((2, chunks, 2, 1, LANES), jnp.float32),
            pltpu.VMEM((8, LANES), jnp.int32),
            pltpu.VMEM((1, up(edge_count, LANES)), jnp.float32),
            pltpu.VMEM((1, up(edge_count, LANES)), jnp.int32),
            pltpu.VMEM((8, cell_count), jnp.int32),
            pltpu.VMEM((8, cell_count), jnp.int32),
            pltpu.VMEM((8, cell_count), jnp.float32),
            pltpu.VMEM(dv_edge.shape, jnp.float32),
            pltpu.VMEM(dc_edge.shape, jnp.float32),
            pltpu.VMEM(cells_on_edge.shape, jnp.int32),
            pltpu.VMEM(edges_on_cell.shape, jnp.int32),
            pltpu.VMEM(send_cells.shape, jnp.int32),
            pltpu.VMEM(cell_area.shape, jnp.float32),
            pltpu.VMEM(level_coef.shape, jnp.float32),
            pltpu.VMEM((up(levels_n, 8), LANES), jnp.float32),
            pltpu.SemaphoreType.DMA((len(gather(parts, cuts)),)),
            pltpu.SemaphoreType.DMA((7,)),
            pltpu.SemaphoreType.DMA((2,)),
            pltpu.SemaphoreType.DMA((2, chunks, 2)),
        ],
        compiler_params=pltpu.CompilerParams(
            collective_id=0,
            has_side_effects=True,
            vmem_limit_bytes=67043328 - fields_n * up(levels_n, 8) * cell_count * 4,
        ),
        name="diffuse",
    )(
        field, dv_edge, dc_edge, cells_on_edge, edges_on_cell, send_cells, cell_area, level_coef
    )


def solution(mesh):
    return jax.shard_map(
        functools.partial(shards, mesh.shape["cells"]),
        mesh=mesh,
        in_specs=(
            P(None, None, "cells"),
            P("cells"),
            P("cells"),
            P("cells"),
            P(None, "cells"),
            P(None, "cells"),
            P(None, "cells"),
            P(),
        ),
        out_specs=P(None, None, "cells"),
        check_vma=False,
    )
```

```python
import functools

import jax
import jax.numpy as jnp
from jax import lax
from jax.experimental import pallas as pl
from jax.experimental.pallas import tpu as pltpu
from jax.sharding import PartitionSpec as P

CELLS_Y = 16
BLOCK_ROW = 16
OFFSETS = (1, -1, BLOCK_ROW, -BLOCK_ROW, BLOCK_ROW - 1, 1 - BLOCK_ROW)
LANES = 128
HALVES = 2
UNIT = 16
CUTS = (7, 8, 8, 8)
ORDER = ((1, 0), (1, 1), (2, 0), (1, 2), (2, 1), (1, 3), (2, 2), (2, 3), (0, 0), (0, 1), (0, 2), (0, 3), (3, 0), (3, 1), (3, 2))


def up(value, step):
    return -(-value // step) * step


def slots(length):
    side = CELLS_Y
    counts = (side, side, length, length, 1, 1)
    order = (2, 3, 0, 1, 4, 5)
    base = [0] * 6
    at = 0
    for k in order:
        base[k] = at
        at += counts[k]
    return tuple(base), counts, at


def layout(fields_n, levels_n):
    stride = up(levels_n, 8)
    whole = levels_n // 8 * 8
    rest = levels_n - whole
    gaps = [
        f * stride + l for f in range(fields_n - 1) for l in range(levels_n, stride)
    ]
    last = (fields_n - 1) * stride
    parts = [(f, 0, levels_n, f * stride) for f in range(fields_n - 1)]
    if rest <= len(gaps) and (last + whole) % UNIT == 0:
        parts.append((fields_n - 1, 0, whole, last))
        parts += [(fields_n - 1, whole + i, 1, gaps[i]) for i in range(rest)]
        return parts, gaps[rest:], last + whole
    parts.append((fields_n - 1, 0, levels_n, last))
    rows = up(last + levels_n, UNIT)
    return parts, gaps + list(range(last + levels_n, rows)), rows


def bounds(rows):
    parts = rows // UNIT
    total = sum(CUTS)
    return [parts * sum(CUTS[:k]) // total * UNIT for k in range(len(CUTS) + 1)]


def gather(parts, cuts):
    groups = []
    for f in range(1 + max(part[0] for part in parts)):
        row = min(part[3] for part in parts if part[0] == f)
        c = max(k for k in range(len(cuts)) if cuts[k] <= row)
        if groups and groups[-1][2] == c:
            groups[-1][1] += 1
        else:
            groups.append([f, 1, c])
    return sorted(groups, key=lambda group: group[2])


def strips(cuts):
    starts = [0]
    for c in range(len(cuts) - 1):
        assert cuts[c + 1] - cuts[c] <= LANES
        starts.append(starts[-1] + cuts[c + 1] - cuts[c] + 2 * CELLS_Y)
    return starts


def split(values):
    high = values.astype(jnp.bfloat16)
    low = (values - high.astype(jnp.float32)).astype(jnp.bfloat16)
    return high, low


def border(strip, corner_a, corner_b, size, length):
    base, counts, _ = slots(length)
    h = size // 2
    left = lax.broadcasted_iota(jnp.int32, (h, LANES), 1) < length
    above = strip[:h]
    below = strip[h:size]
    edge = jnp.concatenate(
        [
            jnp.where(left, above, pltpu.roll(below, length, 1)),
            jnp.where(left, pltpu.roll(above, length, 1), below),
        ],
        axis=0,
    )
    corners = jnp.zeros((LANES - 2 * CELLS_Y, LANES), jnp.float32)
    place = lax.broadcasted_iota(jnp.int32, corners.shape, 0)
    for k, corner in ((4, corner_a), (5, corner_b)):
        value = jnp.broadcast_to(corner, corners.shape)
        corners = jnp.where(place == base[k] - base[4], value, corners)
    small = jnp.concatenate([strip[size:], corners], axis=0)
    high, low = split(jnp.concatenate([edge, small.T[:size]], axis=1))
    return jnp.concatenate([high, low], axis=0)


def split_fields(parts, cuts):
    return min(f for f, _, size, row in parts if row + size > cuts[-2])


def write_kernel(
    length, parts, cuts, head_ref, tail_ref, sum_ref, rim, strip_ref, corner_ref, scale_ref,
    out_hbm, rest, sems,
):
    lead = head_ref.shape[0]
    fields_n, levels_n, cell_count = out_hbm.shape
    start = cuts[-2]
    size = cuts[-1] - start
    halo = rim.shape[0] // 2
    first = [
        pltpu.make_async_copy(
            head_ref.at[f], out_hbm.at[f], sems.at[0]
        )
        for f in range(lead)
    ]
    for copy in first:
        copy.start()
    for f, level, n, row in parts:
        n = min(n, start - row)
        if f >= lead and n > 0:
            rest[f - lead, level : level + n, :] = tail_ref[f - lead, level : level + n, :]
    lhs = border(strip_ref[...], corner_ref[0], corner_ref[1], size, length)
    width = cell_count // HALVES
    for k in range(HALVES):
        here = slice(k * width, (k + 1) * width)
        both = jnp.dot(lhs, rim[:halo, here], preferred_element_type=jnp.float32)
        fine = jnp.dot(lhs[:size], rim[halo:, here], preferred_element_type=jnp.float32)
        total = sum_ref[:, here] + (both[:size] + both[size:] + fine)
        for f, level, n, row in parts:
            lo = max(start, row)
            hi = row + n
            if lo >= hi:
                continue
            at = level + lo - row
            scale = jnp.broadcast_to(scale_ref[at : at + hi - lo, 0:1], (hi - lo, width))
            rest[f - lead, at : at + hi - lo, here] = total[lo - start : hi - start] * scale
        there = pl.ds(k * width, width)
        pltpu.make_async_copy(
            rest.at[:, :, there], out_hbm.at[pl.ds(lead, fields_n - lead), :, there],
            sems.at[1 + k],
        ).start()
    pltpu.make_async_copy(head_ref, out_hbm.at[pl.ds(0, lead)], sems.at[0]).wait()
    for k in range(HALVES):
        there = pl.ds(k * width, width)
        pltpu.make_async_copy(
            rest.at[:, :, there], out_hbm.at[pl.ds(lead, fields_n - lead), :, there],
            sems.at[1 + k],
        ).wait()


def kernel(
    devices,
    field_hbm, dv_hbm, dc_hbm, ends_hbm, edges_hbm, send_hbm, area_hbm, level_hbm,
    head_ref, tail_ref, sum_ref, rim, last_strip, last_corner, scale_ref,
    landed, flat, first, matrix, pair, selector, strip_out, strip_in,
    corner_out, corner_in, lists, weight, packed, index, near_ref, coef_ref,
    dv_ref, dc_ref, ends_ref, edges_ref, send_ref, area_ref, level_ref,
    load_sem, table_sem, send_sem, recv_sem,
):
    fields_n, levels_n, cell_count = field_hbm.shape
    parts, gaps, rows = layout(fields_n, levels_n)
    cuts = bounds(rows)
    chunks = len(cuts) - 1
    starts = strips(cuts)
    halo = rim.shape[0] // 2
    length = send_ref.shape[1]
    edge_count = ends_ref.shape[1]
    base, counts, used = slots(length)
    me = lax.axis_index("cells")
    targets = [lax.rem(me + (o + devices), devices) for o in OFFSETS]
    tiles = cell_count // LANES

    barrier = pltpu.get_barrier_semaphore()
    for target in targets:
        pl.semaphore_signal(
            barrier, inc=1, device_id=(target,), device_id_type=pl.DeviceIdType.MESH
        )

    send_load = pltpu.make_async_copy(send_hbm, send_ref, table_sem.at[0])
    send_load.start()
    groups = gather(parts, cuts)
    loads = [
        pltpu.make_async_copy(
            field_hbm.at[pl.ds(f, n)], landed.at[pl.ds(f, n)], load_sem.at[i]
        )
        for i, (f, n, _) in enumerate(groups)
    ]
    for load, (_, _, first_use) in zip(loads, groups):
        if first_use == 0:
            load.start()
    pairs = (
        (dv_hbm, dv_ref), (dc_hbm, dc_ref), (ends_hbm, ends_ref), (edges_hbm, edges_ref),
        (area_hbm, area_ref), (level_hbm, level_ref),
    )
    tables = [
        pltpu.make_async_copy(a, b, table_sem.at[i + 1]) for i, (a, b) in enumerate(pairs)
    ]
    send_load.wait()
    lists[0:6, 0:length] = send_ref[...]
    table = lists[...]
    lane = lax.broadcasted_iota(jnp.int32, (1, LANES), 1)
    picks = [jnp.full((1, LANES), -1, jnp.int32)] * (halo // LANES)
    for k in range(6):
        tile, at = base[k] // LANES, base[k] % LANES
        moved = pltpu.roll(table, at, 1) if at else table
        inside = (lane >= at) & (lane < at + counts[k])
        picks[tile] = jnp.where(inside, moved[k : k + 1], picks[tile])
    ids = lax.broadcasted_iota(jnp.int32, (LANES, LANES), 0)
    for r in range(tiles):
        for tile in range(halo // LANES):
            hit = ids == picks[tile] - r * LANES
            selector[r * LANES : (r + 1) * LANES, tile * LANES : (tile + 1) * LANES] = (
                jnp.where(hit, 1.0, 0.0).astype(jnp.bfloat16)
            )

    def spread(values, c):
        low_at = cuts[c + 1] - cuts[c]
        high, low = split(values)
        pair[2 * cuts[c] : 2 * cuts[c] + low_at, :] = high
        pair[2 * cuts[c] + low_at : 2 * cuts[c + 1], :] = low

    def places(c):
        h = (cuts[c + 1] - cuts[c]) // 2
        at = starts[c]
        side = at + 2 * h
        return (
            pl.ds(side, CELLS_Y), pl.ds(side + CELLS_Y, CELLS_Y), pl.ds(at, h), pl.ds(at + h, h)
        )

    def copies(lap, c):
        def ends(k):
            if k < 4:
                here = places(c)[k]
                return strip_out.at[lap, here], strip_in.at[lap, here]
            return corner_out.at[lap, c, k - 4], corner_in.at[lap, c, k - 4]

        return [
            pltpu.make_async_remote_copy(
                src_ref=ends(k)[0],
                dst_ref=ends(k)[1],
                send_sem=send_sem.at[k // 4],
                recv_sem=recv_sem.at[lap, c, k // 4],
                device_id=(targets[k],),
                device_id_type=pl.DeviceIdType.MESH,
            )
            for k in (4, 5, 0, 1, 2, 3)
        ]

    def receive(lap, c):
        strip = strip_in.at[lap, pl.ds(starts[c], starts[c + 1] - starts[c])]
        pltpu.make_async_copy(strip, strip, recv_sem.at[lap, c, 0]).wait()
        corner = corner_in.at[lap, c]
        pltpu.make_async_copy(corner, corner, recv_sem.at[lap, c, 1]).wait()

    def send(lap, c):
        size = cuts[c + 1] - cuts[c]
        h = size // 2
        both = jnp.dot(
            pair[2 * cuts[c] : 2 * cuts[c + 1], :],
            selector[...],
            preferred_element_type=jnp.float32,
        )
        both = both[:size] + both[size:]
        edge = both[:, :LANES]
        turned = pltpu.roll(edge, length, 1)
        left = lax.broadcasted_iota(jnp.int32, (h, LANES), 1) < length
        where = places(c)
        strip_out[lap, where[2], :] = jnp.where(left, edge[:h], turned[h:])
        strip_out[lap, where[3], :] = jnp.where(left, turned[:h], edge[h:])
        small = both[:, LANES:]
        if size < LANES:
            fill = jnp.zeros((LANES - size, LANES), jnp.float32)
            small = jnp.concatenate([small, fill], axis=0)
        small = small.T
        for k in (0, 1):
            at = base[k] - LANES
            strip_out[lap, where[k], :] = small[at : at + counts[k]]
        for k in (4, 5):
            at = base[k] - LANES
            corner_out[lap, c, k - 4] = small[at : at + 1]
        for copy in copies(lap, c):
            copy.start()

    def own(c):
        size = cuts[c + 1] - cuts[c]
        at = 2 * cuts[c]
        both = jnp.dot(
            pair[at : at + 2 * size, :],
            matrix[:cell_count, :],
            preferred_element_type=jnp.float32,
        )
        fine = jnp.dot(
            pair[at : at + size, :],
            matrix[cell_count:, :],
            preferred_element_type=jnp.float32,
        )
        return both[:size] + both[size:] + fine

    def outside(lap, c):
        receive(lap, c)
        size = cuts[c + 1] - cuts[c]
        strip = strip_in[lap, starts[c] : starts[c + 1], :]
        lhs = border(strip, corner_in[lap, c, 0], corner_in[lap, c, 1], size, length)
        both = jnp.dot(lhs, rim[:halo, :], preferred_element_type=jnp.float32)
        fine = jnp.dot(lhs[:size], rim[halo:, :], preferred_element_type=jnp.float32)
        return both[:size] + both[size:] + fine

    for c in range(chunks):
        for load, (f, n, first_use) in zip(loads, groups):
            if first_use != c:
                continue
            load.wait()
            for g, level, size, row in parts:
                if f <= g < f + n:
                    flat[row : row + size, :] = landed[g, level : level + size, :]
        if c == 0:
            for load, (_, _, first_use) in zip(loads, groups):
                if first_use:
                    load.start()
            for load in tables:
                load.start()
        spread(flat[cuts[c] : cuts[c + 1], :], c)
        if c == 0:
            pl.semaphore_wait(barrier, len(targets))
        send(0, c)

    for load in tables:
        load.wait()
    edge_tiles = weight.shape[1] // LANES
    weight[...] = jnp.zeros_like(weight)
    packed[...] = jnp.zeros_like(packed)
    index[...] = jnp.zeros_like(index)
    for k in range(edge_tiles):
        part = slice(k * LANES, min((k + 1) * LANES, edge_count))
        weight[0, part] = dv_ref[part] / dc_ref[part]
    packed[:, :edge_count] = ends_ref[0:1, :] + ends_ref[1:2, :] * 4096
    index[0:6, :] = edges_ref[...]
    row = lax.broadcasted_iota(jnp.int32, (8, LANES), 0)
    lane = lax.broadcasted_iota(jnp.int32, (8, LANES), 1)
    for tile in range(tiles):
        here = slice(tile * LANES, (tile + 1) * LANES)
        wanted = index[:, here]
        high = wanted >> 7
        low = wanted & 127
        w = jnp.zeros((8, LANES), jnp.float32)
        p = jnp.zeros((8, LANES), jnp.int32)
        for k in range(edge_tiles):
            part = slice(k * LANES, (k + 1) * LANES)
            wk = jnp.broadcast_to(weight[0:1, part], (8, LANES))
            pk = jnp.broadcast_to(packed[0:1, part], (8, LANES))
            hit = high == k
            w = jnp.where(hit, jnp.take_along_axis(wk, low, axis=1), w)
            p = jnp.where(hit, jnp.take_along_axis(pk, low, axis=1), p)
        lower = p & 4095
        upper = p >> 12
        other = jnp.where(lower == lane + tile * LANES, upper, lower)
        away = other - cell_count
        place = jnp.zeros((8, LANES), jnp.int32)
        for k in range(6):
            inside = (away >= k * length) & (away < (k + 1) * length)
            place = jnp.where(inside, away - k * length + base[k], place)
        near = jnp.where(away < 0, other, cell_count + place)
        share = w / jnp.broadcast_to(area_ref[here], (8, LANES))
        share = jnp.where(row < 6, share, 0.0)
        total = jnp.sum(share, axis=0, keepdims=True)
        near_ref[:, here] = jnp.where(row < 6, near, -1)
        coef_ref[:, here] = jnp.where(row == 6, total, share)
    tall = scale_ref.shape[0]
    r = lax.broadcasted_iota(jnp.int32, (tall, levels_n), 0)
    c = lax.broadcasted_iota(jnp.int32, (tall, levels_n), 1)
    levels = jnp.broadcast_to(level_ref[...].reshape(1, levels_n), (tall, levels_n))
    column = jnp.sum(jnp.where(r == c, -levels, 0.0), axis=1, keepdims=True)
    scale_ref[...] = jnp.broadcast_to(column, (tall, LANES))

    def entries(start, tile):
        here = slice(tile * LANES, (tile + 1) * LANES)
        block = jnp.zeros((LANES, LANES), jnp.float32)
        for j in range(6):
            hit = ids == near_ref[j : j + 1, here] - start
            block = jnp.where(hit, coef_ref[j : j + 1, here], block)
        return split(block)

    def fill(r, carry):
        start = pl.multiple_of(r * LANES, LANES)
        for tile in range(tiles):
            here = slice(tile * LANES, (tile + 1) * LANES)
            high, low = entries(start, tile)
            matrix[pl.ds(start, LANES), here] = high
            matrix[pl.ds(start + cell_count, LANES), here] = low
        return carry

    lax.fori_loop(0, tiles, fill, 0)
    for r in range(halo // LANES):
        for tile in range(tiles):
            here = slice(tile * LANES, (tile + 1) * LANES)
            high, low = entries(cell_count + r * LANES, tile)
            rim[r * LANES : (r + 1) * LANES, here] = high
            rim[halo + r * LANES : halo + (r + 1) * LANES, here] = low

    def start(c):
        part = slice(cuts[c], cuts[c + 1])
        first[part, :] = own(c) - flat[part, :] * coef_ref[6:7, :]

    def relay(c):
        part = slice(cuts[c], cuts[c + 1])
        result = first[part, :] + outside(0, c)
        first[part, :] = result
        spread(result, c)
        send(1, c)

    def inner(c):
        part = slice(cuts[c], cuts[c + 1])
        flat[part, :] = own(c) - first[part, :] * coef_ref[6:7, :]

    lead = head_ref.shape[0]

    def finish(c):
        part = slice(cuts[c], cuts[c + 1])
        flat[part, :] = flat[part, :] + outside(1, c)
        for f, level, size, row in parts:
            lo = max(cuts[c], row)
            hi = min(cuts[c + 1], row + size)
            if lo >= hi:
                continue
            at = level + lo - row
            scale = jnp.broadcast_to(scale_ref[at : at + hi - lo, 0:1], (hi - lo, cell_count))
            where, g = (head_ref, f) if f < lead else (tail_ref, f - lead)
            where[g, at : at + hi - lo, :] = flat[lo:hi, :] * scale

    for step, c in ORDER:
        (inner, start, relay, finish)[step](c)
    c = chunks - 1
    sum_ref[...] = flat[cuts[c] : cuts[c + 1], :]
    receive(1, c)
    last_strip[...] = strip_in[1, starts[c] : starts[c + 1], :]
    last_corner[...] = corner_in[1, c]
    pltpu.make_async_copy(strip_out, strip_out, send_sem.at[0]).wait()
    pltpu.make_async_copy(corner_out, corner_out, send_sem.at[1]).wait()


def shards(
    devices, field, cell_area, dv_edge, dc_edge, cells_on_edge, edges_on_cell, send_cells,
    level_coef,
):
    length = send_cells.shape[1]
    fields_n, levels_n, cell_count = field.shape
    edge_count = dv_edge.shape[0]
    _, _, used = slots(length)
    halo = up(used, LANES)
    parts, _, rows = layout(fields_n, levels_n)
    cuts = bounds(rows)
    chunks = len(cuts) - 1
    tall = strips(cuts)[-1]
    vmem = pl.BlockSpec(memory_space=pltpu.VMEM)
    hbm = pl.BlockSpec(memory_space=pltpu.HBM)
    lead = split_fields(parts, cuts)
    last = cuts[-1] - cuts[-2]
    shapes = (
        pltpu.VMEM((lead, levels_n, cell_count), jnp.float32),
        pltpu.VMEM((fields_n - lead, levels_n, cell_count), jnp.float32),
        pltpu.VMEM((last, cell_count), jnp.float32),
        pltpu.VMEM((2 * halo, cell_count), jnp.bfloat16),
        pltpu.VMEM((last + 2 * CELLS_Y, LANES), jnp.float32),
        pltpu.VMEM((2, 1, LANES), jnp.float32),
        pltpu.VMEM((up(levels_n, 8), LANES), jnp.float32),
    )
    held = (
        fields_n * up(levels_n, 8) * cell_count * 4
        + last * cell_count * 4
        + 4 * halo * cell_count
        + (last + 2 * CELLS_Y) * LANES * 4
        + 2 * 8 * LANES * 4
        + up(levels_n, 8) * LANES * 4
    )
    results = pl.pallas_call(
        functools.partial(kernel, devices),
        out_shape=shapes,
        in_specs=[hbm] * 8,
        out_specs=(vmem,) * len(shapes),
        scratch_shapes=[
            pltpu.VMEM(field.shape, jnp.float32),
            pltpu.VMEM((rows, cell_count), jnp.float32),
            pltpu.VMEM((rows, cell_count), jnp.float32),
            pltpu.VMEM((2 * cell_count, cell_count), jnp.bfloat16),
            pltpu.VMEM((2 * rows, cell_count), jnp.bfloat16),
            pltpu.VMEM((cell_count, halo), jnp.bfloat16),
            pltpu.VMEM((2, tall, LANES), jnp.float32),
            pltpu.VMEM((2, tall, LANES), jnp.float32),
            pltpu.VMEM((2, chunks, 2, 1, LANES), jnp.float32),
            pltpu.VMEM((2, chunks, 2, 1, LANES), jnp.float32),
            pltpu.VMEM((8, LANES), jnp.int32),
            pltpu.VMEM((1, up(edge_count, LANES)), jnp.float32),
            pltpu.VMEM((1, up(edge_count, LANES)), jnp.int32),
            pltpu.VMEM((8, cell_count), jnp.int32),
            pltpu.VMEM((8, cell_count), jnp.int32),
            pltpu.VMEM((8, cell_count), jnp.float32),
            pltpu.VMEM(dv_edge.shape, jnp.float32),
            pltpu.VMEM(dc_edge.shape, jnp.float32),
            pltpu.VMEM(cells_on_edge.shape, jnp.int32),
            pltpu.VMEM(edges_on_cell.shape, jnp.int32),
            pltpu.VMEM(send_cells.shape, jnp.int32),
            pltpu.VMEM(cell_area.shape, jnp.float32),
            pltpu.VMEM(level_coef.shape, jnp.float32),
            pltpu.SemaphoreType.DMA((len(gather(parts, cuts)),)),
            pltpu.SemaphoreType.DMA((7,)),
            pltpu.SemaphoreType.DMA((2,)),
            pltpu.SemaphoreType.DMA((2, chunks, 2)),
        ],
        compiler_params=pltpu.CompilerParams(
            collective_id=0,
            has_side_effects=True,
            vmem_limit_bytes=67043328 - up(held, 1024),
        ),
        name="diffuse",
    )(
        field, dv_edge, dc_edge, cells_on_edge, edges_on_cell, send_cells, cell_area, level_coef
    )
    return pl.pallas_call(
        functools.partial(write_kernel, length, parts, cuts),
        out_shape=jax.ShapeDtypeStruct(field.shape, jnp.float32),
        in_specs=[vmem] * len(shapes),
        out_specs=hbm,
        scratch_shapes=[
            pltpu.VMEM((fields_n - lead, levels_n, cell_count), jnp.float32),
            pltpu.SemaphoreType.DMA((1 + HALVES,)),
        ],
        compiler_params=pltpu.CompilerParams(vmem_limit_bytes=32 * 1024 * 1024),
        name="write",
    )(*results)


def solution(mesh):
    return jax.shard_map(
        functools.partial(shards, mesh.shape["cells"]),
        mesh=mesh,
        in_specs=(
            P(None, None, "cells"),
            P("cells"),
            P("cells"),
            P("cells"),
            P(None, "cells"),
            P(None, "cells"),
            P(None, "cells"),
            P(),
        ),
        out_specs=P(None, None, "cells"),
        check_vma=False,
    )
```

```python
import functools

import jax
import jax.numpy as jnp
from jax import lax
from jax.experimental import pallas as pl
from jax.experimental.pallas import tpu as pltpu
from jax.sharding import PartitionSpec as P

CELLS_Y = 16
BLOCK_ROW = 16
OFFSETS = (1, -1, BLOCK_ROW, -BLOCK_ROW, BLOCK_ROW - 1, 1 - BLOCK_ROW)
LANES = 128
HALVES = 2
UNIT = 16
CUTS = (8, 8, 8, 7)
ORDER = ((1, 0), (1, 1), (2, 0), (1, 2), (2, 1), (1, 3), (2, 2), (0, 0), (2, 3), (0, 1), (0, 2), (0, 3), (3, 0), (3, 1), (3, 2))


def up(value, step):
    return -(-value // step) * step


def slots(length):
    side = CELLS_Y
    counts = (side, side, length, length, 1, 1)
    order = (2, 3, 0, 1, 4, 5)
    base = [0] * 6
    at = 0
    for k in order:
        base[k] = at
        at += counts[k]
    return tuple(base), counts, at


def layout(fields_n, levels_n):
    stride = up(levels_n, 8)
    whole = levels_n // 8 * 8
    rest = levels_n - whole
    gaps = [
        f * stride + l for f in range(fields_n - 1) for l in range(levels_n, stride)
    ]
    last = (fields_n - 1) * stride
    parts = [(f, 0, levels_n, f * stride) for f in range(fields_n - 1)]
    if rest <= len(gaps) and (last + whole) % UNIT == 0:
        parts.append((fields_n - 1, 0, whole, last))
        parts += [(fields_n - 1, whole + i, 1, gaps[i]) for i in range(rest)]
        return parts, gaps[rest:], last + whole
    parts.append((fields_n - 1, 0, levels_n, last))
    rows = up(last + levels_n, UNIT)
    return parts, gaps + list(range(last + levels_n, rows)), rows


def bounds(rows):
    parts = rows // UNIT
    total = sum(CUTS)
    return [parts * sum(CUTS[:k]) // total * UNIT for k in range(len(CUTS) + 1)]


def gather(parts, cuts):
    groups = []
    for f in range(1 + max(part[0] for part in parts)):
        row = min(part[3] for part in parts if part[0] == f)
        c = max(k for k in range(len(cuts)) if cuts[k] <= row)
        if groups and groups[-1][2] == c:
            groups[-1][1] += 1
        else:
            groups.append([f, 1, c])
    return sorted(groups, key=lambda group: group[2])


def strips(cuts):
    starts = [0]
    for c in range(len(cuts) - 1):
        assert cuts[c + 1] - cuts[c] <= LANES
        starts.append(starts[-1] + cuts[c + 1] - cuts[c] + 2 * CELLS_Y)
    return starts


def split(values):
    high = values.astype(jnp.bfloat16)
    low = (values - high.astype(jnp.float32)).astype(jnp.bfloat16)
    return high, low


def border(strip, corner_a, corner_b, size, length):
    base, counts, _ = slots(length)
    h = size // 2
    left = lax.broadcasted_iota(jnp.int32, (h, LANES), 1) < length
    above = strip[:h]
    below = strip[h:size]
    edge = jnp.concatenate(
        [
            jnp.where(left, above, pltpu.roll(below, length, 1)),
            jnp.where(left, pltpu.roll(above, length, 1), below),
        ],
        axis=0,
    )
    corners = jnp.zeros((LANES - 2 * CELLS_Y, LANES), jnp.float32)
    place = lax.broadcasted_iota(jnp.int32, corners.shape, 0)
    for k, corner in ((4, corner_a), (5, corner_b)):
        value = jnp.broadcast_to(corner, corners.shape)
        corners = jnp.where(place == base[k] - base[4], value, corners)
    small = jnp.concatenate([strip[size:], corners], axis=0)
    high, low = split(jnp.concatenate([edge, small.T[:size]], axis=1))
    return jnp.concatenate([high, low], axis=0)


def split_fields(parts, cuts):
    return min(f for f, _, size, row in parts if row + size > cuts[-2])


def write_kernel(
    length, parts, cuts, head_ref, tail_ref, sum_ref, rim, strip_ref, corner_ref, scale_ref,
    out_hbm, rest, sems,
):
    lead = head_ref.shape[0]
    fields_n, levels_n, cell_count = out_hbm.shape
    start = cuts[-2]
    size = cuts[-1] - start
    halo = rim.shape[0] // 2
    first = [
        pltpu.make_async_copy(
            head_ref.at[f], out_hbm.at[f], sems.at[0]
        )
        for f in range(lead)
    ]
    for copy in first:
        copy.start()
    for f, level, n, row in parts:
        n = min(n, start - row)
        if f >= lead and n > 0:
            rest[f - lead, level : level + n, :] = tail_ref[f - lead, level : level + n, :]
    lhs = border(strip_ref[...], corner_ref[0], corner_ref[1], size, length)
    width = cell_count // HALVES
    for k in range(HALVES):
        here = slice(k * width, (k + 1) * width)
        both = jnp.dot(lhs, rim[:halo, here], preferred_element_type=jnp.float32)
        fine = jnp.dot(lhs[:size], rim[halo:, here], preferred_element_type=jnp.float32)
        total = sum_ref[:, here] + (both[:size] + both[size:] + fine)
        for f, level, n, row in parts:
            lo = max(start, row)
            hi = row + n
            if lo >= hi:
                continue
            at = level + lo - row
            scale = jnp.broadcast_to(scale_ref[at : at + hi - lo, 0:1], (hi - lo, width))
            rest[f - lead, at : at + hi - lo, here] = total[lo - start : hi - start] * scale
        there = pl.ds(k * width, width)
        pltpu.make_async_copy(
            rest.at[:, :, there], out_hbm.at[pl.ds(lead, fields_n - lead), :, there],
            sems.at[1 + k],
        ).start()
    pltpu.make_async_copy(head_ref, out_hbm.at[pl.ds(0, lead)], sems.at[0]).wait()
    for k in range(HALVES):
        there = pl.ds(k * width, width)
        pltpu.make_async_copy(
            rest.at[:, :, there], out_hbm.at[pl.ds(lead, fields_n - lead), :, there],
            sems.at[1 + k],
        ).wait()


def kernel(
    devices,
    field_hbm, dv_hbm, dc_hbm, ends_hbm, edges_hbm, send_hbm, area_hbm, level_hbm,
    head_ref, tail_ref, sum_ref, rim, last_strip, last_corner, scale_ref,
    landed, flat, first, matrix, pair, selector, strip_out, strip_in,
    corner_out, corner_in, lists, weight, packed, index, near_ref, coef_ref,
    dv_ref, dc_ref, ends_ref, edges_ref, send_ref, area_ref, level_ref,
    load_sem, table_sem, send_sem, recv_sem,
):
    fields_n, levels_n, cell_count = field_hbm.shape
    parts, gaps, rows = layout(fields_n, levels_n)
    cuts = bounds(rows)
    chunks = len(cuts) - 1
    starts = strips(cuts)
    halo = rim.shape[0] // 2
    length = send_ref.shape[1]
    edge_count = ends_ref.shape[1]
    base, counts, used = slots(length)
    me = lax.axis_index("cells")
    targets = [lax.rem(me + (o + devices), devices) for o in OFFSETS]
    tiles = cell_count // LANES

    barrier = pltpu.get_barrier_semaphore()
    for target in targets:
        pl.semaphore_signal(
            barrier, inc=1, device_id=(target,), device_id_type=pl.DeviceIdType.MESH
        )

    send_load = pltpu.make_async_copy(send_hbm, send_ref, table_sem.at[0])
    send_load.start()
    groups = gather(parts, cuts)
    loads = [
        pltpu.make_async_copy(
            field_hbm.at[pl.ds(f, n)], landed.at[pl.ds(f, n)], load_sem.at[i]
        )
        for i, (f, n, _) in enumerate(groups)
    ]
    for load, (_, _, first_use) in zip(loads, groups):
        if first_use == 0:
            load.start()
    pairs = (
        (dv_hbm, dv_ref), (dc_hbm, dc_ref), (ends_hbm, ends_ref), (edges_hbm, edges_ref),
        (area_hbm, area_ref), (level_hbm, level_ref),
    )
    tables = [
        pltpu.make_async_copy(a, b, table_sem.at[i + 1]) for i, (a, b) in enumerate(pairs)
    ]
    send_load.wait()
    lists[0:6, 0:length] = send_ref[...]
    table = lists[...]
    lane = lax.broadcasted_iota(jnp.int32, (1, LANES), 1)
    picks = [jnp.full((1, LANES), -1, jnp.int32)] * (halo // LANES)
    for k in range(6):
        tile, at = base[k] // LANES, base[k] % LANES
        moved = pltpu.roll(table, at, 1) if at else table
        inside = (lane >= at) & (lane < at + counts[k])
        picks[tile] = jnp.where(inside, moved[k : k + 1], picks[tile])
    ids = lax.broadcasted_iota(jnp.int32, (LANES, LANES), 0)
    for r in range(tiles):
        for tile in range(halo // LANES):
            hit = ids == picks[tile] - r * LANES
            selector[r * LANES : (r + 1) * LANES, tile * LANES : (tile + 1) * LANES] = (
                jnp.where(hit, 1.0, 0.0).astype(jnp.bfloat16)
            )

    def spread(values, c):
        low_at = cuts[c + 1] - cuts[c]
        high, low = split(values)
        pair[2 * cuts[c] : 2 * cuts[c] + low_at, :] = high
        pair[2 * cuts[c] + low_at : 2 * cuts[c + 1], :] = low

    def places(c):
        h = (cuts[c + 1] - cuts[c]) // 2
        at = starts[c]
        side = at + 2 * h
        return (
            pl.ds(side, CELLS_Y), pl.ds(side + CELLS_Y, CELLS_Y), pl.ds(at, h), pl.ds(at + h, h)
        )

    def copies(lap, c):
        def ends(k):
            if k < 4:
                here = places(c)[k]
                return strip_out.at[lap, here], strip_in.at[lap, here]
            return corner_out.at[lap, c, k - 4], corner_in.at[lap, c, k - 4]

        return [
            pltpu.make_async_remote_copy(
                src_ref=ends(k)[0],
                dst_ref=ends(k)[1],
                send_sem=send_sem.at[k // 4],
                recv_sem=recv_sem.at[lap, c, k // 4],
                device_id=(targets[k],),
                device_id_type=pl.DeviceIdType.MESH,
            )
            for k in (4, 5, 0, 1, 2, 3)
        ]

    def receive(lap, c):
        strip = strip_in.at[lap, pl.ds(starts[c], starts[c + 1] - starts[c])]
        pltpu.make_async_copy(strip, strip, recv_sem.at[lap, c, 0]).wait()
        corner = corner_in.at[lap, c]
        pltpu.make_async_copy(corner, corner, recv_sem.at[lap, c, 1]).wait()

    def send(lap, c):
        size = cuts[c + 1] - cuts[c]
        h = size // 2
        both = jnp.dot(
            pair[2 * cuts[c] : 2 * cuts[c + 1], :],
            selector[...],
            preferred_element_type=jnp.float32,
        )
        both = both[:size] + both[size:]
        edge = both[:, :LANES]
        turned = pltpu.roll(edge, length, 1)
        left = lax.broadcasted_iota(jnp.int32, (h, LANES), 1) < length
        where = places(c)
        strip_out[lap, where[2], :] = jnp.where(left, edge[:h], turned[h:])
        strip_out[lap, where[3], :] = jnp.where(left, turned[:h], edge[h:])
        small = both[:, LANES:]
        if size < LANES:
            fill = jnp.zeros((LANES - size, LANES), jnp.float32)
            small = jnp.concatenate([small, fill], axis=0)
        small = small.T
        for k in (0, 1):
            at = base[k] - LANES
            strip_out[lap, where[k], :] = small[at : at + counts[k]]
        for k in (4, 5):
            at = base[k] - LANES
            corner_out[lap, c, k - 4] = small[at : at + 1]
        for copy in copies(lap, c):
            copy.start()

    def own(c):
        size = cuts[c + 1] - cuts[c]
        at = 2 * cuts[c]
        both = jnp.dot(
            pair[at : at + 2 * size, :],
            matrix[:cell_count, :],
            preferred_element_type=jnp.float32,
        )
        fine = jnp.dot(
            pair[at : at + size, :],
            matrix[cell_count:, :],
            preferred_element_type=jnp.float32,
        )
        return both[:size] + both[size:] + fine

    def outside(lap, c):
        receive(lap, c)
        size = cuts[c + 1] - cuts[c]
        strip = strip_in[lap, starts[c] : starts[c + 1], :]
        lhs = border(strip, corner_in[lap, c, 0], corner_in[lap, c, 1], size, length)
        both = jnp.dot(lhs, rim[:halo, :], preferred_element_type=jnp.float32)
        fine = jnp.dot(lhs[:size], rim[halo:, :], preferred_element_type=jnp.float32)
        return both[:size] + both[size:] + fine

    for c in range(chunks):
        for load, (f, n, first_use) in zip(loads, groups):
            if first_use != c:
                continue
            load.wait()
            for g, level, size, row in parts:
                if f <= g < f + n:
                    flat[row : row + size, :] = landed[g, level : level + size, :]
        if c == 0:
            for load, (_, _, first_use) in zip(loads, groups):
                if first_use:
                    load.start()
            for load in tables:
                load.start()
        spread(flat[cuts[c] : cuts[c + 1], :], c)
        if c == 0:
            pl.semaphore_wait(barrier, len(targets))
        send(0, c)

    for load in tables:
        load.wait()
    edge_tiles = weight.shape[1] // LANES
    weight[...] = jnp.zeros_like(weight)
    packed[...] = jnp.zeros_like(packed)
    index[...] = jnp.zeros_like(index)
    for k in range(edge_tiles):
        part = slice(k * LANES, min((k + 1) * LANES, edge_count))
        weight[0, part] = dv_ref[part] / dc_ref[part]
    packed[:, :edge_count] = ends_ref[0:1, :] + ends_ref[1:2, :] * 4096
    index[0:6, :] = edges_ref[...]
    row = lax.broadcasted_iota(jnp.int32, (8, LANES), 0)
    lane = lax.broadcasted_iota(jnp.int32, (8, LANES), 1)
    for tile in range(tiles):
        here = slice(tile * LANES, (tile + 1) * LANES)
        wanted = index[:, here]
        high = wanted >> 7
        low = wanted & 127
        w = jnp.zeros((8, LANES), jnp.float32)
        p = jnp.zeros((8, LANES), jnp.int32)
        for k in range(edge_tiles):
            part = slice(k * LANES, (k + 1) * LANES)
            wk = jnp.broadcast_to(weight[0:1, part], (8, LANES))
            pk = jnp.broadcast_to(packed[0:1, part], (8, LANES))
            hit = high == k
            w = jnp.where(hit, jnp.take_along_axis(wk, low, axis=1), w)
            p = jnp.where(hit, jnp.take_along_axis(pk, low, axis=1), p)
        lower = p & 4095
        upper = p >> 12
        other = jnp.where(lower == lane + tile * LANES, upper, lower)
        away = other - cell_count
        place = jnp.zeros((8, LANES), jnp.int32)
        for k in range(6):
            inside = (away >= k * length) & (away < (k + 1) * length)
            place = jnp.where(inside, away - k * length + base[k], place)
        near = jnp.where(away < 0, other, cell_count + place)
        share = w / jnp.broadcast_to(area_ref[here], (8, LANES))
        share = jnp.where(row < 6, share, 0.0)
        total = jnp.sum(share, axis=0, keepdims=True)
        near_ref[:, here] = jnp.where(row < 6, near, -1)
        coef_ref[:, here] = jnp.where(row == 6, total, share)
    tall = scale_ref.shape[0]
    r = lax.broadcasted_iota(jnp.int32, (tall, levels_n), 0)
    c = lax.broadcasted_iota(jnp.int32, (tall, levels_n), 1)
    levels = jnp.broadcast_to(level_ref[...].reshape(1, levels_n), (tall, levels_n))
    column = jnp.sum(jnp.where(r == c, -levels, 0.0), axis=1, keepdims=True)
    scale_ref[...] = jnp.broadcast_to(column, (tall, LANES))

    def entries(start, tile):
        here = slice(tile * LANES, (tile + 1) * LANES)
        block = jnp.zeros((LANES, LANES), jnp.float32)
        for j in range(6):
            hit = ids == near_ref[j : j + 1, here] - start
            block = jnp.where(hit, coef_ref[j : j + 1, here], block)
        return split(block)

    def fill(r, carry):
        start = pl.multiple_of(r * LANES, LANES)
        for tile in range(tiles):
            here = slice(tile * LANES, (tile + 1) * LANES)
            high, low = entries(start, tile)
            matrix[pl.ds(start, LANES), here] = high
            matrix[pl.ds(start + cell_count, LANES), here] = low
        return carry

    lax.fori_loop(0, tiles, fill, 0)
    for r in range(halo // LANES):
        for tile in range(tiles):
            here = slice(tile * LANES, (tile + 1) * LANES)
            high, low = entries(cell_count + r * LANES, tile)
            rim[r * LANES : (r + 1) * LANES, here] = high
            rim[halo + r * LANES : halo + (r + 1) * LANES, here] = low

    def start(c):
        part = slice(cuts[c], cuts[c + 1])
        first[part, :] = own(c) - flat[part, :] * coef_ref[6:7, :]

    def relay(c):
        part = slice(cuts[c], cuts[c + 1])
        result = first[part, :] + outside(0, c)
        first[part, :] = result
        spread(result, c)
        send(1, c)

    def inner(c):
        part = slice(cuts[c], cuts[c + 1])
        flat[part, :] = own(c) - first[part, :] * coef_ref[6:7, :]

    lead = head_ref.shape[0]

    def finish(c):
        part = slice(cuts[c], cuts[c + 1])
        flat[part, :] = flat[part, :] + outside(1, c)
        for f, level, size, row in parts:
            lo = max(cuts[c], row)
            hi = min(cuts[c + 1], row + size)
            if lo >= hi:
                continue
            at = level + lo - row
            scale = jnp.broadcast_to(scale_ref[at : at + hi - lo, 0:1], (hi - lo, cell_count))
            where, g = (head_ref, f) if f < lead else (tail_ref, f - lead)
            where[g, at : at + hi - lo, :] = flat[lo:hi, :] * scale

    for step, c in ORDER:
        (inner, start, relay, finish)[step](c)
    c = chunks - 1
    sum_ref[...] = flat[cuts[c] : cuts[c + 1], :]
    receive(1, c)
    last_strip[...] = strip_in[1, starts[c] : starts[c + 1], :]
    last_corner[...] = corner_in[1, c]
    pltpu.make_async_copy(strip_out, strip_out, send_sem.at[0]).wait()
    pltpu.make_async_copy(corner_out, corner_out, send_sem.at[1]).wait()


def shards(
    devices, field, cell_area, dv_edge, dc_edge, cells_on_edge, edges_on_cell, send_cells,
    level_coef,
):
    length = send_cells.shape[1]
    fields_n, levels_n, cell_count = field.shape
    edge_count = dv_edge.shape[0]
    _, _, used = slots(length)
    halo = up(used, LANES)
    parts, _, rows = layout(fields_n, levels_n)
    cuts = bounds(rows)
    chunks = len(cuts) - 1
    tall = strips(cuts)[-1]
    vmem = pl.BlockSpec(memory_space=pltpu.VMEM)
    hbm = pl.BlockSpec(memory_space=pltpu.HBM)
    lead = split_fields(parts, cuts)
    last = cuts[-1] - cuts[-2]
    shapes = (
        pltpu.VMEM((lead, levels_n, cell_count), jnp.float32),
        pltpu.VMEM((fields_n - lead, levels_n, cell_count), jnp.float32),
        pltpu.VMEM((last, cell_count), jnp.float32),
        pltpu.VMEM((2 * halo, cell_count), jnp.bfloat16),
        pltpu.VMEM((last + 2 * CELLS_Y, LANES), jnp.float32),
        pltpu.VMEM((2, 1, LANES), jnp.float32),
        pltpu.VMEM((up(levels_n, 8), LANES), jnp.float32),
    )
    held = (
        fields_n * up(levels_n, 8) * cell_count * 4
        + last * cell_count * 4
        + 4 * halo * cell_count
        + (last + 2 * CELLS_Y) * LANES * 4
        + 2 * 8 * LANES * 4
        + up(levels_n, 8) * LANES * 4
    )
    results = pl.pallas_call(
        functools.partial(kernel, devices),
        out_shape=shapes,
        in_specs=[hbm] * 8,
        out_specs=(vmem,) * len(shapes),
        scratch_shapes=[
            pltpu.VMEM(field.shape, jnp.float32),
            pltpu.VMEM((rows, cell_count), jnp.float32),
            pltpu.VMEM((rows, cell_count), jnp.float32),
            pltpu.VMEM((2 * cell_count, cell_count), jnp.bfloat16),
            pltpu.VMEM((2 * rows, cell_count), jnp.bfloat16),
            pltpu.VMEM((cell_count, halo), jnp.bfloat16),
            pltpu.VMEM((2, tall, LANES), jnp.float32),
            pltpu.VMEM((2, tall, LANES), jnp.float32),
            pltpu.VMEM((2, chunks, 2, 1, LANES), jnp.float32),
            pltpu.VMEM((2, chunks, 2, 1, LANES), jnp.float32),
            pltpu.VMEM((8, LANES), jnp.int32),
            pltpu.VMEM((1, up(edge_count, LANES)), jnp.float32),
            pltpu.VMEM((1, up(edge_count, LANES)), jnp.int32),
            pltpu.VMEM((8, cell_count), jnp.int32),
            pltpu.VMEM((8, cell_count), jnp.int32),
            pltpu.VMEM((8, cell_count), jnp.float32),
            pltpu.VMEM(dv_edge.shape, jnp.float32),
            pltpu.VMEM(dc_edge.shape, jnp.float32),
            pltpu.VMEM(cells_on_edge.shape, jnp.int32),
            pltpu.VMEM(edges_on_cell.shape, jnp.int32),
            pltpu.VMEM(send_cells.shape, jnp.int32),
            pltpu.VMEM(cell_area.shape, jnp.float32),
            pltpu.VMEM(level_coef.shape, jnp.float32),
            pltpu.SemaphoreType.DMA((len(gather(parts, cuts)),)),
            pltpu.SemaphoreType.DMA((7,)),
            pltpu.SemaphoreType.DMA((2,)),
            pltpu.SemaphoreType.DMA((2, chunks, 2)),
        ],
        compiler_params=pltpu.CompilerParams(
            collective_id=0,
            has_side_effects=True,
            vmem_limit_bytes=67043328 - up(held, 1024),
        ),
        name="diffuse",
    )(
        field, dv_edge, dc_edge, cells_on_edge, edges_on_cell, send_cells, cell_area, level_coef
    )
    return pl.pallas_call(
        functools.partial(write_kernel, length, parts, cuts),
        out_shape=jax.ShapeDtypeStruct(field.shape, jnp.float32),
        in_specs=[vmem] * len(shapes),
        out_specs=hbm,
        scratch_shapes=[
            pltpu.VMEM((fields_n - lead, levels_n, cell_count), jnp.float32),
            pltpu.SemaphoreType.DMA((1 + HALVES,)),
        ],
        compiler_params=pltpu.CompilerParams(vmem_limit_bytes=32 * 1024 * 1024),
        name="write",
    )(*results)


def solution(mesh):
    return jax.shard_map(
        functools.partial(shards, mesh.shape["cells"]),
        mesh=mesh,
        in_specs=(
            P(None, None, "cells"),
            P("cells"),
            P("cells"),
            P("cells"),
            P(None, "cells"),
            P(None, "cells"),
            P(None, "cells"),
            P(),
        ),
        out_specs=P(None, None, "cells"),
        check_vma=False,
    )
```
